256 devices in a mesh: gx: 4 (over x), gy: 8 (over z), gz: 8 (over y, core).
Axes of the slice: x: 4, y: 4, z: 8, core: 2. Of those that a mesh axis runs over, the one named last changes fastest.
Arguments:
- tile_coords: int32 [3, 4096], P(None, ('gx', 'gy', 'gz')), may hold values from 0 to 31, as said below
- owner_map: int32 [4096], replicated, may hold values from 0 to 4095, as said below
- bin_tile: int32 [14848], P(('gx', 'gy', 'gz')), may hold values from 0 to 4095, as said below
- bin_count: int32 [14848], P(('gx', 'gy', 'gz')), may hold values from 0 to 2048, as said below
- part_cell: int32 [14848, 2048], P(('gx', 'gy', 'gz')), may hold values from 0 to 511
- part_offset: float32 [14848, 3, 2048], P(('gx', 'gy', 'gz')), may hold values from -0.5 to 0.5
- part_velocity: float32 [14848, 3, 2048], P(('gx', 'gy', 'gz')), may hold values from -5 to 5
- part_affine: float32 [14848, 9, 2048], P(('gx', 'gy', 'gz')), may hold values from -5 to 5
- part_mass: float32 [14848, 2048], P(('gx', 'gy', 'gz')), may hold values from 0.5 to 2
Outputs:
- grid_velocity: float32 [3, 2097152], P(None, ('gx', 'gy', 'gz'))
- pressure: float32 [2097152], P(('gx', 'gy', 'gz'))
- particle_velocity: float32 [14848, 3, 2048], P(('gx', 'gy', 'gz'))
The draws below stay inside these ranges and needn't reach their ends.
Inputs may be any that keep to these rules, and one draw needn't show every extreme that they name: `tile_coords`: storage slot s lies on device s // 16 (device index over gx, gy, gz, slowest first). Coordinates are distinct; an active tile that shares a face with a tile stored on a device is stored on the same device or on one whose index differs by one along one mesh axis. `owner_map`: A permutation of the storage slots. `bin_tile`: the 58 bins of a device are first 32 bins whose tiles it stores itself, then 1 bins for each of the 26 offsets (dx, dy, dz) in -1..1 other than (0, 0, 0), in the order dx slowest, dz fastest, whose tiles are stored on the device at that offset of mesh indices. Bins of an offset that leads outside the mesh name some tile and hold no particles. The first bin_count slots of a bin hold its particles. Every device has a bin holding 2048.
All inputs are finite; a program needn't handle non-finite values.
Results may differ from the reference program's by a relative error of at most 0.0024.
The reference program's roundings to bfloat16 on the way count: a program that leaves them out, or rounds other values in their place, can miss the bound.
Values sent between devices are 32-bit elements; how exact they have to be, the bound alone decides.
No kernel may reach another device: no remote copies, remote signals or barrier semaphores. Data moves between devices by JAX's collectives and lax.ppermute only.
A program may use at most 128 MiB of HBM per device.

```python
import math
import jax
import jax.numpy as jnp
import numpy as np
from jax import lax

TILE = 8
HOME = 4
TPD = 16
SELF_BINS = 32
NBR_BINS = 1
PPT = 2048
SWEEPS = 4
CELLS = 512
BINS = 14848
N_GX = 4
N_GY = 8
N_GZ = 8


neighbour_steps = [(along_x, along_y, along_z) for along_x in (-1, 0, 1) for along_y in (-1, 0, 1) for along_z in (-1, 0, 1) if (along_x, along_y, along_z) != (0, 0, 0)]


def world_layout(key):
    base_key = jax.random.fold_in(key, 4242)
    device_total = N_GX * N_GY * N_GZ
    grid_points = np.array([(along_x, along_y, along_z) for along_x in range(HOME) for along_y in range(HOME) for along_z in range(HOME)], dtype=np.int32)
    is_inner = np.all((grid_points >= 1) & (grid_points <= HOME - 2), axis=1)
    interior = jnp.asarray(grid_points[is_inner])
    surface = jnp.asarray(grid_points[~is_inner])
    inner_total = int(is_inner.sum())
    surface_total = grid_points.shape[0] - inner_total
    inner_order = jax.vmap(lambda subkey: jax.random.permutation(subkey, inner_total))(jax.random.split(jax.random.fold_in(base_key, 1), device_total))
    surface_order = jax.vmap(lambda subkey: jax.random.permutation(subkey, surface_total))(jax.random.split(jax.random.fold_in(base_key, 2), device_total))[:, :TPD - inner_total]
    local_places = jnp.concatenate([interior[inner_order], surface[surface_order]], axis=1)
    devices = jnp.arange(device_total, dtype=jnp.int32)
    placing = jnp.stack([devices // (N_GY * N_GZ), devices // N_GZ % N_GY, devices % N_GZ], axis=1)
    home_coords = placing[:, None, :] * HOME + local_places
    swap_axis = jax.random.randint(jax.random.fold_in(base_key, 3), (), 0, 3)
    parity = jax.random.randint(jax.random.fold_in(base_key, 4), (), 0, 2)
    chosen = jax.random.permutation(jax.random.fold_in(base_key, 5), inner_total)[:2]
    extents = jnp.array([N_GX, N_GY, N_GZ], dtype=jnp.int32)
    strides = jnp.array([N_GY * N_GZ, N_GZ, 1], dtype=jnp.int32)
    along_swap = jnp.take(placing, swap_axis, axis=1)
    swap_limit = extents[swap_axis]
    shifted = along_swap - parity
    upward = (shifted >= 0) & (shifted % 2 == 0) & (along_swap + 1 < swap_limit)
    downward = (shifted >= 0) & (shifted % 2 == 1)
    partner = devices + jnp.where(upward, 1, jnp.where(downward, -1, 0)) * strides[swap_axis]
    shuffles = jax.vmap(lambda subkey: jax.random.permutation(subkey, TPD))(jax.random.split(jax.random.fold_in(base_key, 8), device_total)).astype(jnp.int32)
    home_index = shuffles
    moving = (home_index == chosen[0]) | (home_index == chosen[1])
    holder = jnp.where(moving, partner[:, None], devices[:, None])
    stored = (holder * TPD + home_index).reshape(-1).astype(jnp.int32)
    slot_total = device_total * TPD
    owner = jnp.zeros((slot_total,), jnp.int32).at[stored].set(jnp.arange(slot_total, dtype=jnp.int32))
    coords = jnp.transpose(home_coords.reshape(-1, 3)[stored]).astype(jnp.int32)
    tile_order = jax.vmap(lambda subkey: jax.random.permutation(subkey, TPD))(jax.random.split(jax.random.fold_in(base_key, 6), device_total))
    self_pick = tile_order[:, jnp.arange(SELF_BINS, dtype=jnp.int32) % TPD]
    offsets = jnp.array(neighbour_steps, dtype=jnp.int32)
    target = placing[:, None, :] + offsets[None, :, :]
    inside = jnp.all((target >= 0) & (target < extents[None, None, :]), axis=2)
    target_dev = jnp.where(inside, (target[:, :, 0] * N_GY + target[:, :, 1]) * N_GZ + target[:, :, 2], devices[:, None])
    near_pick = jax.random.randint(jax.random.fold_in(base_key, 7), (device_total, 26, NBR_BINS), 0, TPD)
    slot_all = jnp.concatenate([devices[:, None] * TPD + self_pick, (target_dev[:, :, None] * TPD + near_pick).reshape(device_total, 26 * NBR_BINS)], axis=1)
    bin_tiles = stored[slot_all].reshape(-1).astype(jnp.int32)
    bins_dev = SELF_BINS + 26 * NBR_BINS
    counts = jax.random.randint(jax.random.fold_in(base_key, 9), (device_total, bins_dev), PPT * 3 // 5, PPT + 1)
    full_bin = jax.random.randint(jax.random.fold_in(base_key, 10), (device_total, 1), 0, SELF_BINS)
    counts = jnp.where(jnp.arange(bins_dev, dtype=jnp.int32)[None, :] == full_bin, PPT, counts)
    valid_bins = jnp.concatenate([jnp.ones((device_total, SELF_BINS), dtype=bool), jnp.repeat(inside, NBR_BINS, axis=1)], axis=1)
    counts = jnp.where(valid_bins, counts, 0).reshape(-1).astype(jnp.int32)
    return (coords, owner, bin_tiles, counts)


def draw_tile_coords(key, part):
    return world_layout(key)[0]


def draw_owner_map(key, part):
    return world_layout(key)[1]


def draw_bin_tile(key, part):
    return world_layout(key)[2]


def draw_bin_count(key, part):
    return world_layout(key)[3]


def with_ends(result, key, least, high):
    longest = result.shape.index(max(result.shape))
    spots = []
    for shift in (0, 1):
        where = [jax.random.randint(jax.random.fold_in(key, axis), (), 0, length) for axis, length in enumerate(result.shape)]
        where[longest] = (where[longest] + shift) % result.shape[longest]
        spots.append(tuple(where))
    return result.at[spots[0]].set(least).at[spots[1]].set(high)


def block_levels(key, dims, pieces, least, largest):
    gain, own = 1.0, jax.random.fold_in(key, 6)
    for position, shards_of in pieces:
        draws = jnp.exp(jax.random.uniform(jax.random.fold_in(own, position), (shards_of,), jnp.float32, least / len(pieces), largest / len(pieces)))
        gain = gain * jnp.repeat(draws, dims[position] // shards_of).reshape([-1 if axis == position else 1 for axis in range(len(dims))])
    return gain


def scatter_about(rng, shape, deviation, most, pieces=(), kind=jnp.bfloat16):
    values = jax.random.normal(rng, shape, jnp.float32) * deviation
    if len(pieces) > 0:
        values = block_levels(rng, shape, pieces, -0.22, 0.18) * values
    return jnp.clip(values, min=-most, max=most).astype(kind)


def setup_inputs(seed: int = 0) -> dict:
    key_of = jax.random.split(jax.random.key(seed), 10)
    return {
        "tile_coords": draw_tile_coords(jax.random.fold_in(key_of[9], 71), 0),
        "owner_map": draw_owner_map(jax.random.fold_in(key_of[9], 71), 0),
        "bin_tile": draw_bin_tile(jax.random.fold_in(key_of[9], 71), 0),
        "bin_count": draw_bin_count(jax.random.fold_in(key_of[9], 71), 0),
        "part_cell": with_ends(jax.random.randint(key_of[4], (BINS, PPT), 0, CELLS), jax.random.fold_in(key_of[4], 1), 0, CELLS - 1).astype(jnp.int32),
        "part_offset": jnp.clip(jax.random.uniform(key_of[5], (BINS, 3, PPT), jnp.float32, -0.5, 0.5) * block_levels(key_of[5], (BINS, 3, PPT), ((0, 256),), -0.4, 0.0), -0.5, 0.5),
        "part_velocity": scatter_about(key_of[6], (BINS, 3, PPT), 1.0, 5.0, ((0, 256),), jnp.float32),
        "part_affine": scatter_about(key_of[7], (BINS, 9, PPT), 1.0, 5.0, ((0, 256),), jnp.float32),
        "part_mass": jnp.clip(jnp.exp(math.log(2.0) - 1.3862944 * jax.random.uniform(key_of[8], (BINS, PPT), jnp.float32) ** block_levels(key_of[8], (BINS, PPT), ((0, 256),), -0.2, 0.2)), 0.5, 2.0),
    }


gravity_step = 0.5
face_steps = [(1, 0, 0), (-1, 0, 0), (0, 1, 0), (0, -1, 0), (0, 0, 1), (0, 0, -1)]


def deposits(offsets, velocity, affine, masses, living):
    moments = []
    for component in range(3):
        drift_part = velocity[:, component] - (affine[:, 3 * component] * offsets[:, 0] + affine[:, 3 * component + 1] * offsets[:, 1] + affine[:, 3 * component + 2] * offsets[:, 2])
        moments.append(masses * drift_part)
    stacked = jnp.stack([masses] + moments, axis=1)
    return jnp.where(living[:, None, :], stacked, 0.0).astype(jnp.bfloat16)


def lattice_rows(tile_coords):
    extent_x = HOME * N_GX
    extent_y = HOME * N_GY
    extent_z = HOME * N_GZ
    tile_total = tile_coords.shape[1]
    linear = (tile_coords[0] * extent_y + tile_coords[1]) * extent_z + tile_coords[2]
    lookup = jnp.full((extent_x * extent_y * extent_z,), -1, jnp.int32).at[linear].set(jnp.arange(tile_total, dtype=jnp.int32))
    listing = []
    for relative in face_steps:
        shifted_coord = [tile_coords[number] + relative[number] for number in range(3)]
        inside = (shifted_coord[0] >= 0) & (shifted_coord[0] < extent_x) & (shifted_coord[1] >= 0) & (shifted_coord[1] < extent_y) & (shifted_coord[2] >= 0) & (shifted_coord[2] < extent_z)
        address = (jnp.clip(shifted_coord[0], 0, extent_x - 1) * extent_y + jnp.clip(shifted_coord[1], 0, extent_y - 1)) * extent_z + jnp.clip(shifted_coord[2], 0, extent_z - 1)
        listing.append(jnp.where(inside, lookup[address.astype(jnp.int32)], -1).astype(jnp.int32))
    return jnp.stack(listing, axis=1)


def export_faces(values):
    return jnp.stack([values[:, 0], values[:, -1], values[:, :, 0], values[:, :, -1], values[:, :, :, 0], values[:, :, :, -1]], axis=1)


def component_faces(velocity):
    return jnp.stack([velocity[:, 0, 0], velocity[:, 0, -1], velocity[:, 1, :, 0], velocity[:, 1, :, -1], velocity[:, 2, :, :, 0], velocity[:, 2, :, :, -1]], axis=1)


def beside(values, face_table, neighbour_rows, facing):
    direction = facing // 2
    chosen_rows = neighbour_rows[:, facing]
    ghost_layer = jnp.where((chosen_rows >= 0)[:, None, None], face_table[jnp.maximum(chosen_rows, 0), facing], 0.0)
    ghost_layer = jnp.expand_dims(ghost_layer, direction + 1)
    extent = values.shape[1]
    if facing % 2 == 0:
        return jnp.concatenate([lax.slice_in_dim(values, 1, extent, axis=direction + 1), ghost_layer], axis=direction + 1)
    return jnp.concatenate([ghost_layer, lax.slice_in_dim(values, 0, extent - 1, axis=direction + 1)], axis=direction + 1)


def beside_all(values, face_table, neighbour_rows):
    summed = beside(values, face_table, neighbour_rows, 0)
    for facing in range(1, 6):
        summed = summed + beside(values, face_table, neighbour_rows, facing)
    return summed


def reference(tile_coords, owner_map, bin_tile, bin_count, part_cell, part_offset, part_velocity, part_affine, part_mass):
    plane_cells = TILE * TILE
    total_cells = TILE * plane_cells
    tile_total = tile_coords.shape[1]
    owner_slots = owner_map[bin_tile]
    living = lax.broadcasted_iota(jnp.int32, part_cell.shape, 1) < bin_count[:, None]
    amounts = deposits(part_offset, part_velocity, part_affine, part_mass, living)
    places = (owner_slots[:, None] * total_cells + part_cell).astype(jnp.int32)
    spread = jnp.transpose(amounts.astype(jnp.float32), (1, 0, 2)).reshape(4, -1)
    grid_sums = jnp.zeros((4, tile_total * total_cells), jnp.float32).at[:, places.reshape(-1)].add(spread)
    totals = jnp.transpose(grid_sums.reshape(4, tile_total, TILE, TILE, TILE), (1, 0, 2, 3, 4))
    neighbour_rows = lattice_rows(tile_coords)
    masses = totals[:, 0]
    fluid_mask = masses > 0.0
    safe_mass = jnp.where(fluid_mask, masses, 1.0)
    velocity = jnp.where(fluid_mask[:, None], totals[:, 1:] / safe_mass[:, None], 0.0)
    upward = jnp.array([0.0, 1.0, 0.0], dtype=jnp.float32)
    velocity = velocity - gravity_step * fluid_mask.astype(jnp.float32)[:, None] * upward[None, :, None, None, None]
    velocity_table = component_faces(velocity)
    diverge = 0.5 * (beside(velocity[:, 0], velocity_table, neighbour_rows, 0) - beside(velocity[:, 0], velocity_table, neighbour_rows, 1))
    diverge = diverge + 0.5 * (beside(velocity[:, 1], velocity_table, neighbour_rows, 2) - beside(velocity[:, 1], velocity_table, neighbour_rows, 3))
    diverge = diverge + 0.5 * (beside(velocity[:, 2], velocity_table, neighbour_rows, 4) - beside(velocity[:, 2], velocity_table, neighbour_rows, 5))
    pressure = jnp.zeros_like(masses)
    for sweep_number in range(SWEEPS):
        face_table = export_faces(pressure)
        pressure = jnp.where(fluid_mask, (beside_all(pressure, face_table, neighbour_rows) - diverge) / 6.0, 0.0)
    face_table = export_faces(pressure)
    gradient = jnp.stack([0.5 * (beside(pressure, face_table, neighbour_rows, 2 * component) - beside(pressure, face_table, neighbour_rows, 2 * component + 1)) for component in range(3)], axis=1)
    velocity = jnp.where(fluid_mask[:, None], velocity - gradient, 0.0)
    flat_velocity = jnp.transpose(velocity, (1, 0, 2, 3, 4)).reshape(3, tile_total * total_cells)
    sampled = jnp.transpose(flat_velocity[:, places], (1, 0, 2))
    particle_velocity = jnp.where(living[:, None, :], sampled, 0.0)
    return flat_velocity, pressure.reshape(-1), particle_velocity
```

```python
import jax
import jax.numpy as jnp
from jax import lax
from jax.experimental import pallas as pl
from jax.experimental.pallas import tpu as pltpu
from jax.sharding import PartitionSpec as P

TPD = 16
OWN_BINS = 32
NBR_BINS = 26
BINS = OWN_BINS + NBR_BINS
PPT = 2048
CELLS = 512
LANES = 128
UPPER = CELLS // LANES
REC = 16
GROUP = 9
META = GROUP * REC
PAYLOAD = META + 16
SWEEPS = 4
AXES = ("gx", "gy", "gz")
face_codes = (4096, -4096, 64, -64, 1, -1)


def ring(block, axis, distance):
    size = lax.axis_size(axis)
    return lax.ppermute(block, axis, [(i, (i + distance) % size) for i in range(size)])


def swap(block, axis, which):
    size = lax.axis_size(axis)
    pairs = [(i, ((i + which) ^ 1) - which) for i in range(size)]
    return lax.ppermute(block, axis, [(i, j % size) for i, j in pairs])


def scalars():
    return pl.BlockSpec(memory_space=pltpu.SMEM)


def held():
    return pl.BlockSpec(memory_space=pltpu.VMEM)


def near(values):
    return pltpu.with_memory_space_constraint(values, pltpu.VMEM)


def array(*shape, dtype=jnp.float32):
    return pltpu.VMEM(shape, dtype)


def call(body, name, args, outs, flops=2_000_000, **extra):
    if "grid" not in extra:
        args = [near(arg) for arg in args]
        extra["in_specs"] = [held() for _ in args]
        extra["out_specs"] = tuple(held() for _ in outs) if isinstance(outs, tuple) else held()
    return pl.pallas_call(
        body,
        out_shape=outs,
        name=name,
        cost_estimate=pl.CostEstimate(flops=flops, transcendentals=0, bytes_accessed=500_000),
        **extra,
    )(*args)


def upper_and_hot(cell_ref, row, count):
    cells = cell_ref[row : row + 1, :]
    living = lax.broadcasted_iota(jnp.int32, (1, PPT), 1) < count
    upper = jnp.where(living, cells >> 7, -1)
    lower = cells & (LANES - 1)
    hot = (lax.broadcasted_iota(jnp.int32, (LANES, PPT), 0) == lower).astype(jnp.bfloat16)
    return upper, hot


def store_deposits(off, vel, aff, mass, amounts):
    masses = mass[...]
    amounts[0] = masses.astype(jnp.bfloat16).astype(jnp.float32)
    for a in range(3):
        drift = vel[a] - (aff[3 * a] * off[0] + aff[3 * a + 1] * off[1] + aff[3 * a + 2] * off[2])
        amounts[a + 1] = (masses * drift).astype(jnp.bfloat16).astype(jnp.float32)


def splat_row(cell, amounts, row, count):
    upper, hot = upper_and_hot(cell, row, count)
    position = lax.broadcasted_iota(jnp.int32, (8, PPT), 0)
    first = position == upper
    second = position == jnp.where(upper < 0, -1, upper + UPPER)
    halves = []
    for pair in range(2):
        one = amounts[2 * pair, row : row + 1, :]
        two = amounts[2 * pair + 1, row : row + 1, :]
        halves.append(jnp.where(first, one, jnp.where(second, two, 0.0)))
    weighted = jnp.concatenate(halves, axis=0).astype(jnp.bfloat16)
    return lax.dot_general(
        weighted, hot, (((1,), (1,)), ((), ())), preferred_element_type=jnp.float32
    )


def particle_specs(start):
    return [
        pl.BlockSpec((8, PPT), lambda i: (i + start, 0)),
        pl.BlockSpec((3, 8, PPT), lambda i: (0, i + start, 0)),
        pl.BlockSpec((3, 8, PPT), lambda i: (0, i + start, 0)),
        pl.BlockSpec((9, 8, PPT), lambda i: (0, i + start, 0)),
        pl.BlockSpec((8, PPT), lambda i: (i + start, 0)),
    ]


def splat_own(counts, slots, parts, start, blocks):
    def body(counts, slots, cell, off, vel, aff, mass, acc, amounts):
        @pl.when(pl.program_id(0) == 0)
        def _():
            acc[...] = jnp.zeros_like(acc)

        store_deposits(off, vel, aff, mass, amounts)
        base = (pl.program_id(0) + start) * 8
        summed = [splat_row(cell, amounts, row, counts[base + row]) for row in range(8)]
        for row in range(8):
            place = pl.multiple_of(slots[base + row] * REC, REC)
            acc[pl.ds(place, REC), :] += summed[row]

    return call(
        body,
        "splat_own",
        (counts, slots, *parts),
        array(TPD * REC, LANES),
        flops=blocks * 8 * 2_000_000,
        grid=(blocks,),
        in_specs=[scalars(), scalars()] + particle_specs(start),
        out_specs=held(),
        scratch_shapes=[pltpu.VMEM((4, 8, PPT), jnp.float32)],
    )


def splat_nbr(tile_coords, owner_map, bin_tile, counts, parts):
    first_block = OWN_BINS // 8
    blocks = -(-NBR_BINS // 8)
    last = NBR_BINS - 8 * (blocks - 1)

    def body(coords, owners, bin_tile, counts, cell, off, vel, aff, mass, *rest):
        slots, code_row, code_column, slot_rows, below, middle, above, rec, amounts = rest
        step = pl.program_id(0)

        @pl.when(step == 0)
        def _():
            for number in range(BINS):
                slots[number] = owners[bin_tile[number]] & (TPD - 1)
            for number in range(NBR_BINS):
                value = slots[OWN_BINS + number].astype(jnp.float32)
                slot_rows[number : number + 1, :] = jnp.full((1, LANES), value, jnp.float32)
            turn_of = lax.broadcasted_iota(jnp.int32, (8, LANES), 1) & (TPD - 1)
            row_of = lax.broadcasted_iota(jnp.int32, (TPD, LANES), 0)
            along, down = jnp.zeros((8, LANES), jnp.int32), jnp.zeros((TPD, LANES), jnp.int32)
            for t in range(TPD):
                code = (coords[0, t] + 1) * 4096 + (coords[1, t] + 1) * 64 + coords[2, t] + 1
                along = jnp.where(turn_of == t, code, along)
                down = jnp.where(row_of == t, code, down)
            code_row[...] = along.astype(jnp.float32)
            code_column[...] = down.astype(jnp.float32)

        store_deposits(off, vel, aff, mass, amounts)

        def splat(rows):
            for row in range(rows):
                number = step * 8 + row
                rec[pl.ds(pl.multiple_of(number * REC, REC), REC), :] = splat_row(
                    cell, amounts, row, counts[OWN_BINS + number]
                )

        @pl.when(step < blocks - 1)
        def _():
            splat(8)

        @pl.when(step == blocks - 1)
        def _():
            splat(last)
            for out, begin in ((below, 0), (above, 17)):
                out[0:META, :] = rec[begin * REC : (begin + GROUP) * REC, :]
                out[META : META + GROUP, :] = slot_rows[begin : begin + GROUP, :]
                out[META + GROUP : META + GROUP + 1, :] = code_row[0:1, :]
                out[META + GROUP + 1 : PAYLOAD, :] = jnp.zeros((6, LANES), jnp.float32)
            middle[...] = rec[GROUP * REC : 17 * REC, :]

    return call(
        body,
        "splat_nbr",
        (tile_coords, owner_map, bin_tile, counts, *parts),
        (
            jax.ShapeDtypeStruct((BINS,), jnp.int32),
            array(8, LANES),
            array(TPD, LANES),
            array(32, LANES),
            array(PAYLOAD, LANES),
            array(8 * REC, LANES),
            array(PAYLOAD, LANES),
        ),
        flops=NBR_BINS * 2_000_000,
        grid=(blocks,),
        in_specs=[scalars()] * 4 + particle_specs(first_block),
        out_specs=(scalars(),) + (held(),) * 6,
        scratch_shapes=[
            pltpu.VMEM((NBR_BINS * REC, LANES), jnp.float32),
            pltpu.VMEM((4, 8, PPT), jnp.float32),
        ],
    )


middle_steps = [(b, c) for b in (-1, 0, 1) for c in (-1, 0, 1) if (b, c) != (0, 0)]


def mid_of(dy, dz):
    return ("mid", middle_steps.index((dy, dz)))


def y_sources(orient):
    listing = [mid_of(orient, dz) for dz in (-1, 0, 1)]
    for arrived in ("xp", "xm"):
        listing += [(arrived, (orient + 1) * 3 + dz + 1) for dz in (-1, 0, 1)]
    return listing


def z_sources(orient):
    listing = [mid_of(0, orient)]
    listing += [(arrived, 3 + orient + 1) for arrived in ("xp", "xm")]
    for arrived in ("yp", "ym"):
        listing += [(arrived, 3 * group + orient + 1) for group in range(3)]
    return listing


consumed = (
    [("zp", n) for n in range(9)]
    + [("zm", n) for n in range(9)]
    + [("yp", 3 * g + 1) for g in range(3)]
    + [("ym", 3 * g + 1) for g in range(3)]
    + [("xp", 4), ("xm", 4)]
)


def y_reply_sources(sign):
    local, offset = (18, 3) if sign > 0 else (21, 6)
    listing = []
    for g in range(3):
        listing += [("zm", offset + g), ("rec", local + g), ("zp", offset + g)]
    return listing


def x_reply_sources(sign):
    group = 1 if sign > 0 else 2
    local = ("rec", 24 if sign > 0 else 25)
    return (
        [("ym", 3 * group + n) for n in range(3)]
        + [("zm", group), local, ("zp", group)]
        + [("yp", 3 * group + n) for n in range(3)]
    )


final_sources = (
    [("xm", n) for n in range(9)]
    + [("ym", n) for n in range(3)]
    + [("zm", 0), ("zp", 0)]
    + [("yp", n) for n in range(3)]
    + [("xp", n) for n in range(9)]
)


def record(ref, number):
    return ref[number * REC : (number + 1) * REC, :]


def slot_row(refs, source, slot_rows):
    name, number = source
    if name == "mid":
        return slot_rows[GROUP + number : GROUP + number + 1, :]
    return refs[name][META + number : META + number + 1, :]


def forward(names, buffers, slot_rows, code_row, sources, title):
    def body(*refs):
        kept = dict(zip(names, refs))
        slots, codes = refs[len(names)], refs[len(names) + 1]
        for out, listing in zip(refs[len(names) + 2 :], sources):
            for number, source in enumerate(listing):
                out[number * REC : (number + 1) * REC, :] = record(kept[source[0]], source[1])
                out[META + number : META + number + 1, :] = slot_row(kept, source, slots)
            out[META + GROUP : META + GROUP + 1, :] = codes[0:1, :]
            out[META + GROUP + 1 : PAYLOAD, :] = jnp.zeros((6, LANES), jnp.float32)

    payload = array(PAYLOAD, LANES)
    return call(body, title, (*buffers, slot_rows, code_row), (payload, payload))


def reply(names, buffers, sources, title):
    def body(*refs):
        kept = dict(zip(names, refs))
        for out, listing in zip(refs[len(names) :], sources):
            for number, source in enumerate(listing):
                out[number * REC : (number + 1) * REC, :] = record(kept[source[0]], source[1])

    payload = array(META, LANES)
    return call(body, title, tuple(buffers), (payload, payload))


def thirds(values):
    high = values.astype(jnp.bfloat16)
    rest = values - high.astype(jnp.float32)
    middle = rest.astype(jnp.bfloat16)
    low = (rest - middle.astype(jnp.float32)).astype(jnp.bfloat16)
    return high, middle, low


def pick(hot, values):
    found = None
    for part in thirds(values):
        term = lax.dot_general(
            hot, part, (((1,), (0,)), ((), ())), preferred_element_type=jnp.float32
        )
        found = term if found is None else found + term
    return found


def cell_axes():
    lane = lax.broadcasted_iota(jnp.int32, (TPD, CELLS), 1)
    return lane >> 6, (lane >> 3) & 7, lane & 7


def turn(values, shift):
    return pltpu.roll(values, shift % CELLS, 1)


def beside(values, ghost, facing):
    axis, step = facing // 2, (64, 8, 1)[facing // 2]
    index = cell_axes()[axis]
    if facing % 2 == 0:
        return jnp.where(index == 7, turn(ghost, 7 * step), turn(values, -step))
    return jnp.where(index == 0, turn(ghost, -7 * step), turn(values, step))


def table_of(refs, begin):
    rows = [ref[:, begin : begin + CELLS] for ref in refs]
    return jnp.concatenate(rows + [jnp.zeros((LANES - 7 * TPD, CELLS), jnp.float32)], axis=0)


def ghosts_of(hot, refs):
    found = pick(hot, table_of(refs, 0))
    return [found[TPD * facing : TPD * (facing + 1)] for facing in range(6)]


def gather_grid(arrivals, accs):
    names = ("xp", "xm", "yp", "ym", "zp", "zm")

    def body(*refs):
        kept = dict(zip(names, refs[:6]))
        own = refs[6 : 6 + len(accs)]
        velocity, fluid_out, slots_out, rec = refs[6 + len(accs) :]
        for number, source in enumerate(consumed):
            rec[number * REC : (number + 1) * REC, :] = record(kept[source[0]], source[1])
            slots_out[number : number + 1, :] = slot_row(kept, source, None)
        rec[NBR_BINS * REC : 32 * REC, :] = jnp.zeros(((32 - NBR_BINS) * REC, LANES), jnp.float32)
        slots_out[NBR_BINS:32, :] = jnp.full((32 - NBR_BINS, LANES), -1.0, jnp.float32)
        hot = (
            slots_out[...] == lax.broadcasted_iota(jnp.int32, (32, LANES), 1).astype(jnp.float32)
        ).astype(jnp.float32)
        hot = jnp.transpose(hot)[:TPD, :].astype(jnp.bfloat16)
        received = jnp.concatenate([rec[pl.ds(r, 32, stride=REC), :] for r in range(REC)], axis=1)
        totals = pick(hot, received)
        for acc in own:
            totals = totals + jnp.concatenate(
                [acc[pl.ds(r, TPD, stride=REC), :] for r in range(REC)], axis=1
            )
        masses = totals[:, :CELLS]
        fluid = masses > 0.0
        safe = jnp.where(fluid, masses, 1.0)
        for a in range(3):
            value = totals[:, (a + 1) * CELLS : (a + 2) * CELLS] / safe
            if a == 1:
                value = value - 0.5
            velocity[:, a * CELLS : (a + 1) * CELLS] = jnp.where(fluid, value, 0.0)
        fluid_out[...] = fluid.astype(jnp.float32)

    return call(
        body,
        "gather_grid",
        (*arrivals, *accs),
        (
            array(TPD, 3 * CELLS),
            array(TPD, CELLS),
            array(32, LANES),
        ),
        scratch_shapes=[pltpu.VMEM((32 * REC, LANES), jnp.float32)],
    )


def divergence(arrivals, code_row, code_column, velocity, fluid, arrived):
    def body(*refs):
        payloads, code_row, code_column, fluid = refs[:6], refs[6], refs[7], refs[8]
        fields = refs[9:16]
        hot_out, div_out, pressure = refs[16:]
        group = lax.broadcasted_iota(jnp.int32, (1, LANES), 1) // TPD
        codes = jnp.where(group == 0, code_row[0:1, :], -9999.0)
        for number, ref in enumerate(payloads):
            odd = lax.axis_index(AXES[number // 2]) & 1
            slot = 2 * (number // 2) + 2 - (number + odd) % 2
            codes = jnp.where(group == slot, ref[META + GROUP : META + GROUP + 1, :], codes)
        hots = [
            (code_column[...] + float(step) == codes).astype(jnp.bfloat16) for step in face_codes
        ]
        hot = jnp.concatenate(hots, axis=0)
        hot_out[...] = hot
        total = None
        for a in range(3):
            table = table_of(fields, a * CELLS)
            found = pick(hot[2 * a * TPD : (2 * a + 2) * TPD], table)
            own = fields[0][:, a * CELLS : (a + 1) * CELLS]
            term = 0.5 * (beside(own, found[:TPD], 2 * a) - beside(own, found[TPD:], 2 * a + 1))
            total = term if total is None else total + term
        div_out[...] = total
        pressure[...] = jnp.where(fluid[...] > 0.0, (0.0 - total) / 6.0, 0.0)

    field = array(TPD, CELLS)
    return call(
        body,
        "divergence",
        (*arrivals, code_row, code_column, fluid, velocity, *arrived),
        (array(6 * TPD, LANES, dtype=jnp.bfloat16), field, field),
    )


def sweep(hot, div, fluid, pressure, arrived):
    def body(hot, div, fluid, *refs):
        fields, out = refs[:7], refs[7]
        values = fields[0][...]
        total = None
        for facing, ghost in enumerate(ghosts_of(hot[...], fields)):
            term = beside(values, ghost, facing)
            total = term if total is None else total + term
        out[...] = jnp.where(fluid[...] > 0.0, (total - div[...]) / 6.0, 0.0)

    return call(
        body,
        "sweep",
        (hot, div, fluid, pressure, *arrived),
        array(TPD, CELLS),
    )


def project(hot, fluid, velocity, slots, pressure, arrived):
    def body(hot, fluid, velocity, slots, *refs):
        fields = refs[:7]
        grid_out, tiles, back_p, back_m, back_local, rec = refs[7:]
        values = fields[0][...]
        ghosts = ghosts_of(hot[...], fields)
        wet = fluid[...] > 0.0
        tiles[...] = jnp.zeros_like(tiles)
        rec[...] = jnp.zeros_like(rec)
        named = (
            slots[...] == lax.broadcasted_iota(jnp.int32, (32, LANES), 1).astype(jnp.float32)
        ).astype(jnp.bfloat16)[:, :TPD]
        for a in range(3):
            slope = 0.5 * (
                beside(values, ghosts[2 * a], 2 * a) - beside(values, ghosts[2 * a + 1], 2 * a + 1)
            )
            final = jnp.where(wet, velocity[:, a * CELLS : (a + 1) * CELLS] - slope, 0.0)
            grid_out[a] = final
            copies = pick(named, final)
            for u in range(UPPER):
                row = a * UPPER + u
                tiles[pl.ds(row, TPD, stride=REC), :] = final[:, u * LANES : (u + 1) * LANES]
                rec[pl.ds(row, 32, stride=REC), :] = copies[:, u * LANES : (u + 1) * LANES]
        back_p[...] = rec[:META, :]
        back_m[...] = rec[META : 2 * META, :]
        back_local[...] = rec[2 * META : NBR_BINS * REC, :]

    block = array(META, LANES)
    return call(
        body,
        "project",
        (hot, fluid, velocity, slots, pressure, *arrived),
        (
            array(3, TPD, CELLS),
            array(TPD * REC, LANES),
            block,
            block,
            array(8 * REC, LANES),
        ),
        scratch_shapes=[pltpu.VMEM((32 * REC, LANES), jnp.float32)],
    )


def sample_row(cell, out, tile, row, count):
    upper, hot = upper_and_hot(cell, row, count)
    high = tile.astype(jnp.bfloat16)
    low = (tile - high.astype(jnp.float32)).astype(jnp.bfloat16)
    planes = lax.dot_general(
        jnp.concatenate([high, low], axis=0),
        hot,
        (((1,), (0,)), ((), ())),
        preferred_element_type=jnp.float32,
    )
    planes = planes[:REC] + planes[REC:]
    wanted = (lax.broadcasted_iota(jnp.int32, (8, PPT), 0) & (UPPER - 1)) == upper
    sums = []
    for half in range(2):
        kept = jnp.where(wanted, planes[8 * half : 8 * half + 8], 0.0)
        kept = kept + pltpu.roll(kept, 7, 0)
        sums.append(kept + pltpu.roll(kept, 6, 0))
    out[0, row : row + 1, :] = sums[0][0:1]
    out[1, row : row + 1, :] = sums[0][4:5]
    out[2, row : row + 1, :] = sums[1][0:1]


particle_shape = jax.ShapeDtypeStruct((3, BINS, PPT), jnp.float32)


def sample_own(counts, slots, cell, tiles, sampled, start, blocks):
    def body(counts, slots, cell, tiles, *refs):
        out = refs[-1]
        base = (pl.program_id(0) + start) * 8

        for row in range(8):
            place = pl.multiple_of(slots[base + row] * REC, REC)
            sample_row(cell, out, tiles[pl.ds(place, REC), :], row, counts[base + row])

    args = [counts, slots, cell, near(tiles)]
    specs = [
        scalars(),
        scalars(),
        pl.BlockSpec((8, PPT), lambda i: (i + start, 0)),
        held(),
    ]
    alias = {}
    if sampled is not None:
        args.append(sampled)
        specs.append(pl.BlockSpec(memory_space=pl.ANY))
        alias = {4: 0}
    return call(
        body,
        "sample_own",
        tuple(args),
        particle_shape,
        flops=blocks * 8 * 2_000_000,
        grid=(blocks,),
        in_specs=specs,
        out_specs=pl.BlockSpec((3, 8, PPT), lambda i: (0, i + start, 0)),
        input_output_aliases=alias,
    )


def sample_nbr(counts, cell, buffers, sampled):
    names = ("xp", "xm", "yp", "ym", "zp", "zm")
    first_block = OWN_BINS // 8
    blocks = -(-NBR_BINS // 8)

    def body(counts, cell, *refs):
        kept = dict(zip(names, refs[:6]))
        out, rec = refs[7:]
        step = pl.program_id(0)

        @pl.when(step == 0)
        def _():
            for number, source in enumerate(final_sources):
                rec[number * REC : (number + 1) * REC, :] = record(kept[source[0]], source[1])

        def sample(rows):
            for row in range(rows):
                number = step * 8 + row
                place = pl.multiple_of(number * REC, REC)
                sample_row(cell, out, rec[pl.ds(place, REC), :], row, counts[OWN_BINS + number])

        @pl.when(step < blocks - 1)
        def _():
            sample(8)

        @pl.when(step == blocks - 1)
        def _():
            sample(NBR_BINS - 8 * (blocks - 1))

    return call(
        body,
        "sample_nbr",
        (counts, cell, *[near(buffer) for buffer in buffers], sampled),
        particle_shape,
        flops=NBR_BINS * 2_000_000,
        grid=(blocks,),
        in_specs=[scalars(), pl.BlockSpec((8, PPT), lambda i: (i + first_block, 0))]
        + [held()] * 6
        + [pl.BlockSpec(memory_space=pl.ANY)],
        out_specs=pl.BlockSpec((3, 8, PPT), lambda i: (0, i + first_block, 0)),
        input_output_aliases={8: 0},
        scratch_shapes=[pltpu.VMEM((NBR_BINS * REC, LANES), jnp.float32)],
    )


def exchange(values):
    return [swap(values, axis, which) for axis in AXES for which in (0, 1)]


def together(*values):
    return lax.optimization_barrier(values)


def with_kept(sources):
    return [("kept", n - 18) if name == "rec" else (name, n) for name, n in sources]


def local(tile_coords, owner_map, bin_tile, counts, cell, offset, velocity, affine, mass):
    parts = (
        cell,
        jnp.transpose(offset, (1, 0, 2)),
        jnp.transpose(velocity, (1, 0, 2)),
        jnp.transpose(affine, (1, 0, 2)),
        mass,
    )
    slots, code_row, code_column, slot_rows, below, middle, above = splat_nbr(
        tile_coords, owner_map, bin_tile, counts, parts
    )
    xp, xm = ring(above, "gx", 1), ring(below, "gx", -1)
    acc_x = splat_own(counts, slots, parts, 0, 2)
    xp, xm, acc_x = together(xp, xm, acc_x)
    up, down = forward(
        ("mid", "xp", "xm"),
        (middle, xp, xm),
        slot_rows,
        code_row,
        (y_sources(1), y_sources(-1)),
        "forward_y",
    )
    slots, up, down = together(slots, up, down)
    yp, ym = ring(up, "gy", 1), ring(down, "gy", -1)
    acc_y = splat_own(counts, slots, parts, 2, 1)
    yp, ym, acc_y = together(yp, ym, acc_y)
    up, down = forward(
        ("mid", "xp", "xm", "yp", "ym"),
        (middle, xp, xm, yp, ym),
        slot_rows,
        code_row,
        (z_sources(1), z_sources(-1)),
        "forward_z",
    )
    slots, up, down = together(slots, up, down)
    zp, zm = ring(up, "gz", 1), ring(down, "gz", -1)
    acc_z = splat_own(counts, slots, parts, 3, 1)
    arrivals = (xp, xm, yp, ym, zp, zm)
    grid_u, fluid, nbr_slots = gather_grid(arrivals, (acc_x, acc_y, acc_z))
    hot, div, pressure = divergence(
        arrivals, code_row, code_column, grid_u, fluid, exchange(grid_u)
    )
    for _ in range(SWEEPS - 1):
        pressure = sweep(hot, div, fluid, pressure, exchange(pressure))
    grid_v, tiles, back_p, back_m, kept = project(
        hot, fluid, grid_u, nbr_slots, pressure, exchange(pressure)
    )
    rzp, rzm = ring(back_p, "gz", -1), ring(back_m, "gz", 1)
    sampled = sample_own(counts, slots, cell, tiles, None, 0, 2)
    rzp, rzm, sampled = together(rzp, rzm, sampled)
    up, down = reply(
        ("kept", "zp", "zm"),
        (kept, rzp, rzm),
        (with_kept(y_reply_sources(1)), with_kept(y_reply_sources(-1))),
        "reply_y",
    )
    slots, up, down = together(slots, up, down)
    ryp, rym = ring(up, "gy", -1), ring(down, "gy", 1)
    sampled = sample_own(counts, slots, cell, tiles, sampled, 2, 1)
    ryp, rym, sampled = together(ryp, rym, sampled)
    up, down = reply(
        ("kept", "zp", "zm", "yp", "ym"),
        (kept, rzp, rzm, ryp, rym),
        (with_kept(x_reply_sources(1)), with_kept(x_reply_sources(-1))),
        "reply_x",
    )
    slots, up, down = together(slots, up, down)
    rxp, rxm = ring(up, "gx", -1), ring(down, "gx", 1)
    sampled = sample_own(counts, slots, cell, tiles, sampled, 3, 1)
    sampled = sample_nbr(counts, cell, (rxp, rxm, ryp, rym, rzp, rzm), sampled)
    return (
        grid_v.reshape(3, TPD * CELLS),
        pressure.reshape(-1),
        jnp.transpose(sampled, (1, 0, 2)),
    )


def solution(mesh):
    split = P(AXES)
    particles = P(AXES, None, None)
    return jax.shard_map(
        local,
        mesh=mesh,
        in_specs=(
            P(None, AXES),
            P(),
            split,
            split,
            P(AXES, None),
            particles,
            particles,
            particles,
            P(AXES, None),
        ),
        out_specs=(P(None, AXES), split, particles),
        check_vma=False,
    )
```

```python
import jax
import jax.numpy as jnp
from jax import lax
from jax.experimental import pallas as pl
from jax.experimental.pallas import tpu as pltpu
from jax.sharding import PartitionSpec as P

TPD = 16
OWN_BINS = 32
NBR_BINS = 26
BINS = OWN_BINS + NBR_BINS
PPT = 2048
CELLS = 512
LANES = 128
UPPER = CELLS // LANES
REC = 16
GROUP = 9
META = GROUP * REC
PAYLOAD = META + 16
SWEEPS = 4
AXES = ("gx", "gy", "gz")
face_codes = (4096, -4096, 64, -64, 1, -1)


def ring(block, axis, distance):
    size = lax.axis_size(axis)
    return lax.ppermute(block, axis, [(i, (i + distance) % size) for i in range(size)])


def swap(block, axis, which):
    size = lax.axis_size(axis)
    pairs = [(i, ((i + which) ^ 1) - which) for i in range(size)]
    return lax.ppermute(block, axis, [(i, j % size) for i, j in pairs])


def scalars():
    return pl.BlockSpec(memory_space=pltpu.SMEM)


def held():
    return pl.BlockSpec(memory_space=pltpu.VMEM)


def near(values):
    return pltpu.with_memory_space_constraint(values, pltpu.VMEM)


def array(*shape, dtype=jnp.float32):
    return pltpu.VMEM(shape, dtype)


def call(body, name, args, outs, flops=2_000_000, **extra):
    if "grid" not in extra:
        args = [near(arg) for arg in args]
        extra["in_specs"] = [held() for _ in args]
        extra["out_specs"] = tuple(held() for _ in outs) if isinstance(outs, tuple) else held()
    return pl.pallas_call(
        body,
        out_shape=outs,
        name=name,
        cost_estimate=pl.CostEstimate(flops=flops, transcendentals=0, bytes_accessed=500_000),
        **extra,
    )(*args)


def one_hot(cells, width):
    lower = (cells & (width - 1)).astype(jnp.float32).astype(jnp.bfloat16)
    index = lax.broadcasted_iota(jnp.int32, (width, PPT), 0).astype(jnp.float32)
    return jnp.where(index.astype(jnp.bfloat16) == lower, jnp.bfloat16(1), jnp.bfloat16(0))


def upper_index(cells, width, count):
    living = lax.broadcasted_iota(jnp.int32, (1, PPT), 1) < count
    return jnp.where(living, cells >> (width.bit_length() - 1), -1)


def store_deposits(off, vel, aff, mass, amounts):
    masses = mass[...]
    amounts[0] = masses.astype(jnp.bfloat16).astype(jnp.float32)
    for a in range(3):
        drift = vel[a] - (aff[3 * a] * off[0] + aff[3 * a + 1] * off[1] + aff[3 * a + 2] * off[2])
        amounts[a + 1] = (masses * drift).astype(jnp.bfloat16).astype(jnp.float32)


def splat_row(cell, amounts, row, count):
    half = LANES // 2
    cells = cell[row : row + 1, :]
    upper = upper_index(cells, half, count)
    position = lax.broadcasted_iota(jnp.int32, (8, PPT), 0)
    chosen = [
        jnp.where(
            position < UPPER,
            amounts[2 * pair, row : row + 1, :],
            amounts[2 * pair + 1, row : row + 1, :],
        )
        for pair in range(2)
    ]
    weighted = []
    for side in range(2):
        there = 2 * (position & (UPPER - 1)) + side == upper
        weighted += [jnp.where(there, values, 0.0) for values in chosen]
    summed = lax.dot_general(
        jnp.concatenate(weighted, axis=0).astype(jnp.bfloat16),
        one_hot(cells, half),
        (((1,), (1,)), ((), ())),
        preferred_element_type=jnp.float32,
    )
    return jnp.concatenate([summed[:REC], summed[REC:]], axis=1)


def particle_specs(start):
    return [
        pl.BlockSpec((8, PPT), lambda i: (i + start, 0)),
        pl.BlockSpec((3, 8, PPT), lambda i: (0, i + start, 0)),
        pl.BlockSpec((3, 8, PPT), lambda i: (0, i + start, 0)),
        pl.BlockSpec((9, 8, PPT), lambda i: (0, i + start, 0)),
        pl.BlockSpec((8, PPT), lambda i: (i + start, 0)),
    ]


def splat_own(counts, slots, parts, start, blocks):
    def body(counts, slots, cell, off, vel, aff, mass, acc, amounts):
        @pl.when(pl.program_id(0) == 0)
        def _():
            acc[...] = jnp.zeros_like(acc)

        store_deposits(off, vel, aff, mass, amounts)
        base = (pl.program_id(0) + start) * 8
        summed = [splat_row(cell, amounts, row, counts[base + row]) for row in range(8)]
        for row in range(8):
            place = pl.multiple_of(slots[base + row] * REC, REC)
            acc[pl.ds(place, REC), :] += summed[row]

    return call(
        body,
        "splat_own",
        (counts, slots, *parts),
        array(TPD * REC, LANES),
        flops=blocks * 8 * 2_000_000,
        grid=(blocks,),
        in_specs=[scalars(), scalars()] + particle_specs(start),
        out_specs=held(),
        scratch_shapes=[pltpu.VMEM((4, 8, PPT), jnp.float32)],
    )


FIRST = OWN_BINS // 8
side_rows = (tuple(range(8)), (0,), tuple(range(1, 8)), (0, 1))
middle_rows = {1: tuple(range(1, 8)), 2: (0,)}


def side_place(number):
    return (0, number) if number < GROUP else (1, number - 17)


def splat_sides(tile_coords, owner_map, bin_tile, counts, parts):
    def body(coords, owners, bin_tile, counts, cell, off, vel, aff, mass, *rest):
        slots, code_row, code_column, slot_rows, below, above, amounts = rest
        step = pl.program_id(0)

        @pl.when(step == 0)
        def _():
            for number in range(BINS):
                slots[number] = owners[bin_tile[number]] & (TPD - 1)
            for number in range(NBR_BINS):
                value = slots[OWN_BINS + number].astype(jnp.float32)
                slot_rows[number : number + 1, :] = jnp.full((1, LANES), value, jnp.float32)
            turn_of = lax.broadcasted_iota(jnp.int32, (8, LANES), 1) & (TPD - 1)
            row_of = lax.broadcasted_iota(jnp.int32, (TPD, LANES), 0)
            along, down = jnp.zeros((8, LANES), jnp.int32), jnp.zeros((TPD, LANES), jnp.int32)
            for t in range(TPD):
                code = (coords[0, t] + 1) * 4096 + (coords[1, t] + 1) * 64 + coords[2, t] + 1
                along = jnp.where(turn_of == t, code, along)
                down = jnp.where(row_of == t, code, down)
            code_row[...] = along.astype(jnp.float32)
            code_column[...] = down.astype(jnp.float32)
            for out, begin in ((below, 0), (above, 17)):
                out[META : META + GROUP, :] = slot_rows[begin : begin + GROUP, :]
                out[META + GROUP : META + GROUP + 1, :] = code_row[0:1, :]
                out[META + GROUP + 1 : PAYLOAD, :] = jnp.zeros((6, LANES), jnp.float32)

        store_deposits(off, vel, aff, mass, amounts)

        def splat(block, rows):
            @pl.when(step == block)
            def _():
                for row in rows:
                    number = block * 8 + row
                    way, index = side_place(number)
                    out = (below, above)[way]
                    out[index * REC : (index + 1) * REC, :] = splat_row(
                        cell, amounts, row, counts[OWN_BINS + number]
                    )

        for block, rows in enumerate(side_rows):
            splat(block, rows)

    return call(
        body,
        "splat_sides",
        (tile_coords, owner_map, bin_tile, counts, *parts),
        (
            pltpu.SMEM((BINS,), jnp.int32),
            array(8, LANES),
            array(TPD, LANES),
            array(32, LANES),
            array(PAYLOAD, LANES),
            array(PAYLOAD, LANES),
        ),
        flops=18 * 2_000_000,
        grid=(len(side_rows),),
        in_specs=[scalars()] * 4 + particle_specs(FIRST),
        out_specs=(scalars(),) + (held(),) * 5,
        scratch_shapes=[pltpu.VMEM((4, 8, PPT), jnp.float32)],
    )


def splat_middle(counts, slots, parts):
    def body(counts, slots, cell, off, vel, aff, mass, middle, amounts):
        store_deposits(off, vel, aff, mass, amounts)

        def splat(block, rows):
            @pl.when(pl.program_id(0) == block - 1)
            def _():
                for row in rows:
                    number = block * 8 + row
                    index = number - GROUP
                    middle[index * REC : (index + 1) * REC, :] = splat_row(
                        cell, amounts, row, counts[OWN_BINS + number]
                    )

        for block, rows in middle_rows.items():
            splat(block, rows)

    return call(
        body,
        "splat_middle",
        (counts, slots, *parts),
        array(8 * REC, LANES),
        flops=8 * 2_000_000,
        grid=(2,),
        in_specs=[scalars(), scalars()] + particle_specs(FIRST + 1),
        out_specs=held(),
        scratch_shapes=[pltpu.VMEM((4, 8, PPT), jnp.float32)],
    )


middle_steps = [(b, c) for b in (-1, 0, 1) for c in (-1, 0, 1) if (b, c) != (0, 0)]


def mid_of(dy, dz):
    return ("mid", middle_steps.index((dy, dz)))


def y_sources(orient):
    listing = [mid_of(orient, dz) for dz in (-1, 0, 1)]
    for arrived in ("xp", "xm"):
        listing += [(arrived, (orient + 1) * 3 + dz + 1) for dz in (-1, 0, 1)]
    return listing


def z_sources(orient):
    listing = [mid_of(0, orient)]
    listing += [(arrived, 3 + orient + 1) for arrived in ("xp", "xm")]
    for arrived in ("yp", "ym"):
        listing += [(arrived, 3 * group + orient + 1) for group in range(3)]
    return listing


consumed = (
    [("zp", n) for n in range(9)]
    + [("zm", n) for n in range(9)]
    + [("yp", 3 * g + 1) for g in range(3)]
    + [("ym", 3 * g + 1) for g in range(3)]
    + [("xp", 4), ("xm", 4)]
)


def y_reply_sources(sign):
    local, offset = (18, 3) if sign > 0 else (21, 6)
    listing = []
    for g in range(3):
        listing += [("zm", offset + g), ("rec", local + g), ("zp", offset + g)]
    return listing


def x_reply_sources(sign):
    group = 1 if sign > 0 else 2
    local = ("rec", 24 if sign > 0 else 25)
    return (
        [("ym", 3 * group + n) for n in range(3)]
        + [("zm", group), local, ("zp", group)]
        + [("yp", 3 * group + n) for n in range(3)]
    )


final_sources = (
    [("xm", n) for n in range(9)]
    + [("ym", n) for n in range(3)]
    + [("zm", 0), ("zp", 0)]
    + [("yp", n) for n in range(3)]
    + [("xp", n) for n in range(9)]
)


def record(ref, number):
    return ref[number * REC : (number + 1) * REC, :]


def slot_row(refs, source, slot_rows):
    name, number = source
    if name == "mid":
        return slot_rows[GROUP + number : GROUP + number + 1, :]
    return refs[name][META + number : META + number + 1, :]


def forward(names, buffers, slot_rows, code_row, sources, title):
    def body(*refs):
        kept = dict(zip(names, refs))
        slots, codes = refs[len(names)], refs[len(names) + 1]
        for out, listing in zip(refs[len(names) + 2 :], sources):
            for number, source in enumerate(listing):
                out[number * REC : (number + 1) * REC, :] = record(kept[source[0]], source[1])
                out[META + number : META + number + 1, :] = slot_row(kept, source, slots)
            out[META + GROUP : META + GROUP + 1, :] = codes[0:1, :]
            out[META + GROUP + 1 : PAYLOAD, :] = jnp.zeros((6, LANES), jnp.float32)

    payload = array(PAYLOAD, LANES)
    return call(body, title, (*buffers, slot_rows, code_row), (payload, payload))


def reply(names, buffers, sources, title):
    def body(*refs):
        kept = dict(zip(names, refs))
        for out, listing in zip(refs[len(names) :], sources):
            for number, source in enumerate(listing):
                out[number * REC : (number + 1) * REC, :] = record(kept[source[0]], source[1])

    payload = array(META, LANES)
    return call(body, title, tuple(buffers), (payload, payload))


def thirds(values):
    high = values.astype(jnp.bfloat16)
    rest = values - high.astype(jnp.float32)
    middle = rest.astype(jnp.bfloat16)
    low = (rest - middle.astype(jnp.float32)).astype(jnp.bfloat16)
    return high, middle, low


def pick(hot, values):
    found = None
    for part in thirds(values):
        term = lax.dot_general(
            hot, part, (((1,), (0,)), ((), ())), preferred_element_type=jnp.float32
        )
        found = term if found is None else found + term
    return found


def cell_axes():
    lane = lax.broadcasted_iota(jnp.int32, (TPD, CELLS), 1)
    return lane >> 6, (lane >> 3) & 7, lane & 7


def turn(values, shift):
    return pltpu.roll(values, shift % CELLS, 1)


def beside(values, ghost, facing):
    axis, step = facing // 2, (64, 8, 1)[facing // 2]
    index = cell_axes()[axis]
    if facing % 2 == 0:
        return jnp.where(index == 7, turn(ghost, 7 * step), turn(values, -step))
    return jnp.where(index == 0, turn(ghost, -7 * step), turn(values, step))


def table_of(refs, begin):
    rows = [ref[:, begin : begin + CELLS] for ref in refs]
    return jnp.concatenate(rows + [jnp.zeros((LANES - 7 * TPD, CELLS), jnp.float32)], axis=0)


def ghosts_of(hot, refs):
    found = pick(hot, table_of(refs, 0))
    return [found[TPD * facing : TPD * (facing + 1)] for facing in range(6)]


def gather_grid(arrivals, accs):
    names = ("xp", "xm", "yp", "ym", "zp", "zm")

    def body(*refs):
        kept = dict(zip(names, refs[:6]))
        own = refs[6 : 6 + len(accs)]
        velocity, fluid_out, slots_out, rec = refs[6 + len(accs) :]
        for number, source in enumerate(consumed):
            rec[number * REC : (number + 1) * REC, :] = record(kept[source[0]], source[1])
            slots_out[number : number + 1, :] = slot_row(kept, source, None)
        rec[NBR_BINS * REC : 32 * REC, :] = jnp.zeros(((32 - NBR_BINS) * REC, LANES), jnp.float32)
        slots_out[NBR_BINS:32, :] = jnp.full((32 - NBR_BINS, LANES), -1.0, jnp.float32)
        hot = (
            slots_out[...] == lax.broadcasted_iota(jnp.int32, (32, LANES), 1).astype(jnp.float32)
        ).astype(jnp.float32)
        hot = jnp.transpose(hot)[:TPD, :].astype(jnp.bfloat16)
        received = jnp.concatenate([rec[pl.ds(r, 32, stride=REC), :] for r in range(REC)], axis=1)
        totals = pick(hot, received)
        for acc in own:
            totals = totals + jnp.concatenate(
                [acc[pl.ds(r, TPD, stride=REC), :] for r in range(REC)], axis=1
            )
        masses = totals[:, :CELLS]
        fluid = masses > 0.0
        safe = jnp.where(fluid, masses, 1.0)
        for a in range(3):
            value = totals[:, (a + 1) * CELLS : (a + 2) * CELLS] / safe
            if a == 1:
                value = value - 0.5
            velocity[:, a * CELLS : (a + 1) * CELLS] = jnp.where(fluid, value, 0.0)
        fluid_out[...] = fluid.astype(jnp.float32)

    return call(
        body,
        "gather_grid",
        (*arrivals, *accs),
        (
            array(TPD, 3 * CELLS),
            array(TPD, CELLS),
            array(32, LANES),
        ),
        scratch_shapes=[pltpu.VMEM((32 * REC, LANES), jnp.float32)],
    )


def divergence(arrivals, code_row, code_column, velocity, fluid, arrived):
    def body(*refs):
        payloads, code_row, code_column, fluid = refs[:6], refs[6], refs[7], refs[8]
        fields = refs[9:16]
        hot_out, div_out, pressure = refs[16:]
        group = lax.broadcasted_iota(jnp.int32, (1, LANES), 1) // TPD
        codes = jnp.where(group == 0, code_row[0:1, :], -9999.0)
        for number, ref in enumerate(payloads):
            odd = lax.axis_index(AXES[number // 2]) & 1
            slot = 2 * (number // 2) + 2 - (number + odd) % 2
            codes = jnp.where(group == slot, ref[META + GROUP : META + GROUP + 1, :], codes)
        hots = [
            (code_column[...] + float(step) == codes).astype(jnp.bfloat16) for step in face_codes
        ]
        hot = jnp.concatenate(hots, axis=0)
        hot_out[...] = hot
        total = None
        for a in range(3):
            table = table_of(fields, a * CELLS)
            found = pick(hot[2 * a * TPD : (2 * a + 2) * TPD], table)
            own = fields[0][:, a * CELLS : (a + 1) * CELLS]
            term = 0.5 * (beside(own, found[:TPD], 2 * a) - beside(own, found[TPD:], 2 * a + 1))
            total = term if total is None else total + term
        div_out[...] = total
        pressure[...] = jnp.where(fluid[...] > 0.0, (0.0 - total) / 6.0, 0.0)

    field = array(TPD, CELLS)
    return call(
        body,
        "divergence",
        (*arrivals, code_row, code_column, fluid, velocity, *arrived),
        (array(6 * TPD, LANES, dtype=jnp.bfloat16), field, field),
    )


def sweep(hot, div, fluid, pressure, arrived):
    def body(hot, div, fluid, *refs):
        fields, out = refs[:7], refs[7]
        values = fields[0][...]
        total = None
        for facing, ghost in enumerate(ghosts_of(hot[...], fields)):
            term = beside(values, ghost, facing)
            total = term if total is None else total + term
        out[...] = jnp.where(fluid[...] > 0.0, (total - div[...]) / 6.0, 0.0)

    return call(
        body,
        "sweep",
        (hot, div, fluid, pressure, *arrived),
        array(TPD, CELLS),
    )


def project(hot, fluid, velocity, slots, pressure, arrived):
    def body(hot, fluid, velocity, slots, *refs):
        fields = refs[:7]
        tiles, back_p, back_m, back_local, rec = refs[7:]
        values = fields[0][...]
        ghosts = ghosts_of(hot[...], fields)
        wet = fluid[...] > 0.0
        tiles[...] = jnp.zeros_like(tiles)
        rec[...] = jnp.zeros_like(rec)
        named = (
            slots[...] == lax.broadcasted_iota(jnp.int32, (32, LANES), 1).astype(jnp.float32)
        ).astype(jnp.bfloat16)[:, :TPD]
        for a in range(3):
            slope = 0.5 * (
                beside(values, ghosts[2 * a], 2 * a) - beside(values, ghosts[2 * a + 1], 2 * a + 1)
            )
            final = jnp.where(wet, velocity[:, a * CELLS : (a + 1) * CELLS] - slope, 0.0)
            copies = pick(named, final)
            for u in range(UPPER):
                row = a * UPPER + u
                tiles[pl.ds(row, TPD, stride=REC), :] = final[:, u * LANES : (u + 1) * LANES]
                rec[pl.ds(row, 32, stride=REC), :] = copies[:, u * LANES : (u + 1) * LANES]
        back_p[...] = rec[:META, :]
        back_m[...] = rec[META : 2 * META, :]
        back_local[...] = rec[2 * META : NBR_BINS * REC, :]

    block = array(META, LANES)
    return call(
        body,
        "project",
        (hot, fluid, velocity, slots, pressure, *arrived),
        (
            array(TPD * REC, LANES),
            block,
            block,
            array(8 * REC, LANES),
        ),
        scratch_shapes=[pltpu.VMEM((32 * REC, LANES), jnp.float32)],
    )


def results(tiles, pressure):
    def body(tiles, pressure, grid_out, pressure_out):
        for t in range(TPD):
            for u in range(UPPER):
                begin = t * CELLS + u * LANES
                grid_out[:, begin : begin + LANES] = tiles[pl.ds(t * REC + u, 3, stride=UPPER), :]
        for u in range(UPPER):
            pressure_out[pl.ds(u, TPD, stride=UPPER), :] = pressure[:, u * LANES : (u + 1) * LANES]

    return call(
        body,
        "results",
        (tiles, pressure),
        (array(3, TPD * CELLS), array(TPD * UPPER, LANES)),
    )


def sample_row(cell, tile, row, count):
    cells = cell[row : row + 1, :]
    upper = upper_index(cells, LANES, count)
    high = tile.astype(jnp.bfloat16)
    low = (tile - high.astype(jnp.float32)).astype(jnp.bfloat16)
    planes = lax.dot_general(
        jnp.concatenate([high, low], axis=0),
        one_hot(cells, LANES),
        (((1,), (0,)), ((), ())),
        preferred_element_type=jnp.float32,
    )
    planes = planes[:REC] + planes[REC:]
    wanted = (lax.broadcasted_iota(jnp.int32, (8, PPT), 0) & (UPPER - 1)) == upper
    sums = []
    for half in range(2):
        kept = jnp.where(wanted, planes[8 * half : 8 * half + 8], 0.0)
        kept = kept + pltpu.roll(kept, 7, 0)
        sums.append(kept + pltpu.roll(kept, 6, 0))
    return sums[0][0:1], sums[0][4:5], sums[1][0:1]


def store_row(out, row, values):
    for a in range(3):
        out[a, row : row + 1, :] = values[a]


particle_shape = jax.ShapeDtypeStruct((3, BINS, PPT), jnp.float32)


def sample_own(counts, slots, cell, tiles, sampled, start, blocks):
    def body(counts, slots, cell, tiles, *refs):
        out = refs[-1]
        base = (pl.program_id(0) + start) * 8
        for row in range(8):
            place = pl.multiple_of(slots[base + row] * REC, REC)
            tile = tiles[pl.ds(place, REC), :]
            store_row(out, row, sample_row(cell, tile, row, counts[base + row]))

    args = [counts, slots, cell, near(tiles)]
    specs = [
        scalars(),
        scalars(),
        pl.BlockSpec((8, PPT), lambda i: (i + start, 0)),
        held(),
    ]
    alias = {}
    if sampled is not None:
        args.append(sampled)
        specs.append(pl.BlockSpec(memory_space=pl.ANY))
        alias = {4: 0}
    return call(
        body,
        "sample_own",
        tuple(args),
        particle_shape,
        flops=blocks * 8 * 2_000_000,
        grid=(blocks,),
        in_specs=specs,
        out_specs=pl.BlockSpec((3, 8, PPT), lambda i: (0, i + start, 0)),
        input_output_aliases=alias,
    )


def sample_middle(counts, slots, cell, buffers):
    names = ("yp", "ym", "zp", "zm")

    def body(counts, slots, cell, *refs):
        held_by = dict(zip(names, refs))
        out = refs[len(names)]

        def sample(block, rows):
            @pl.when(pl.program_id(0) == block - 1)
            def _():
                for row in rows:
                    number = block * 8 + row
                    name, index = final_sources[number]
                    values = sample_row(
                        cell, record(held_by[name], index), row, counts[OWN_BINS + number]
                    )
                    store_row(out, number - GROUP, values)

        for block, rows in middle_rows.items():
            sample(block, rows)

    return call(
        body,
        "sample_middle",
        (counts, slots, cell, *[near(buffer) for buffer in buffers]),
        array(3, 8, PPT),
        flops=8 * 2_000_000,
        grid=(2,),
        in_specs=[scalars(), scalars(), pl.BlockSpec((8, PPT), lambda i: (i + FIRST + 1, 0))]
        + [held()] * len(names),
        out_specs=held(),
    )


def sample_sides(counts, cell, buffers, middle, sampled):
    def body(counts, cell, xp, xm, middle, sampled, out):
        held_by = {"xp": xp, "xm": xm}

        def sample(block, rows):
            @pl.when(pl.program_id(0) == block)
            def _():
                for row in rows:
                    number = block * 8 + row
                    name, index = final_sources[number]
                    values = sample_row(
                        cell, record(held_by[name], index), row, counts[OWN_BINS + number]
                    )
                    store_row(out, row, values)
                for row in middle_rows.get(block, ()):
                    index = block * 8 + row - GROUP
                    store_row(out, row, [middle[a, index : index + 1, :] for a in range(3)])

        for block, rows in enumerate(side_rows):
            sample(block, rows)

    return call(
        body,
        "sample_sides",
        (counts, cell, *[near(value) for value in (*buffers, middle)], sampled),
        particle_shape,
        flops=18 * 2_000_000,
        grid=(len(side_rows),),
        in_specs=[scalars(), pl.BlockSpec((8, PPT), lambda i: (i + FIRST, 0))]
        + [held()] * 3
        + [pl.BlockSpec(memory_space=pl.ANY)],
        out_specs=pl.BlockSpec((3, 8, PPT), lambda i: (0, i + FIRST, 0)),
        input_output_aliases={5: 0},
    )


def exchange(values):
    got = {(axis, which): swap(values, axis, which) for which in (0, 1) for axis in AXES}
    return [got[axis, which] for axis in AXES for which in (0, 1)]


def together(*values):
    return lax.optimization_barrier(values)


def with_kept(sources):
    return [("kept", n - 18) if name == "rec" else (name, n) for name, n in sources]


def local(tile_coords, owner_map, bin_tile, counts, cell, offset, velocity, affine, mass):
    parts = (
        cell,
        jnp.transpose(offset, (1, 0, 2)),
        jnp.transpose(velocity, (1, 0, 2)),
        jnp.transpose(affine, (1, 0, 2)),
        mass,
    )
    slots, code_row, code_column, slot_rows, below, above = splat_sides(
        tile_coords, owner_map, bin_tile, counts, parts
    )
    xp, xm = ring(above, "gx", 1), ring(below, "gx", -1)
    middle = splat_middle(counts, slots, parts)
    up, down = forward(
        ("mid", "xp", "xm"),
        (middle, xp, xm),
        slot_rows,
        code_row,
        (y_sources(1), y_sources(-1)),
        "forward_y",
    )
    slots, up, down = together(slots, up, down)
    yp, ym = ring(up, "gy", 1), ring(down, "gy", -1)
    acc_y = splat_own(counts, slots, parts, 0, 2)
    yp, ym, acc_y = together(yp, ym, acc_y)
    up, down = forward(
        ("mid", "xp", "xm", "yp", "ym"),
        (middle, xp, xm, yp, ym),
        slot_rows,
        code_row,
        (z_sources(1), z_sources(-1)),
        "forward_z",
    )
    slots, up, down = together(slots, up, down)
    zp, zm = ring(up, "gz", 1), ring(down, "gz", -1)
    acc_z = splat_own(counts, slots, parts, 2, 2)
    arrivals = (xp, xm, yp, ym, zp, zm)
    grid_u, fluid, nbr_slots = gather_grid(arrivals, (acc_y, acc_z))
    hot, div, pressure = divergence(
        arrivals, code_row, code_column, grid_u, fluid, exchange(grid_u)
    )
    for _ in range(SWEEPS - 1):
        pressure = sweep(hot, div, fluid, pressure, exchange(pressure))
    tiles, back_p, back_m, kept = project(
        hot, fluid, grid_u, nbr_slots, pressure, exchange(pressure)
    )
    rzp, rzm = ring(back_p, "gz", -1), ring(back_m, "gz", 1)
    sampled = sample_own(counts, slots, cell, tiles, None, 0, 2)
    rzp, rzm, sampled = together(rzp, rzm, sampled)
    up, down = reply(
        ("kept", "zp", "zm"),
        (kept, rzp, rzm),
        (with_kept(y_reply_sources(1)), with_kept(y_reply_sources(-1))),
        "reply_y",
    )
    slots, up, down = together(slots, up, down)
    ryp, rym = ring(up, "gy", -1), ring(down, "gy", 1)
    sampled = sample_own(counts, slots, cell, tiles, sampled, 2, 2)
    ryp, rym, sampled = together(ryp, rym, sampled)
    up, down = reply(
        ("kept", "zp", "zm", "yp", "ym"),
        (kept, rzp, rzm, ryp, rym),
        (with_kept(x_reply_sources(1)), with_kept(x_reply_sources(-1))),
        "reply_x",
    )
    slots, up, down = together(slots, up, down)
    rxp, rxm = ring(up, "gx", -1), ring(down, "gx", 1)
    middle = sample_middle(counts, slots, cell, (ryp, rym, rzp, rzm))
    grid_v, final_pressure = results(tiles, pressure)
    sampled = sample_sides(counts, cell, (rxp, rxm), middle, sampled)
    return grid_v, final_pressure.reshape(-1), jnp.transpose(sampled, (1, 0, 2))


def solution(mesh):
    split = P(AXES)
    particles = P(AXES, None, None)
    return jax.shard_map(
        local,
        mesh=mesh,
        in_specs=(
            P(None, AXES),
            P(),
            split,
            split,
            P(AXES, None),
            particles,
            particles,
            particles,
            P(AXES, None),
        ),
        out_specs=(P(None, AXES), split, particles),
        check_vma=False,
    )
```

```python
import jax
import jax.numpy as jnp
from jax import lax
from jax.experimental import pallas as pl
from jax.experimental.pallas import tpu as pltpu
from jax.sharding import PartitionSpec as P

TPD = 16
OWN_BINS = 32
NBR_BINS = 26
BINS = OWN_BINS + NBR_BINS
PPT = 2048
CELLS = 512
LANES = 128
UPPER = CELLS // LANES
REC = 16
GROUP = 9
META = GROUP * REC
PAYLOAD = META + 16
SWEEPS = 4
AXES = ("gx", "gy", "gz")
OWNERS = 4096
FACES = CELLS + 2 * LANES
face_codes = (4096, -4096, 64, -64, 1, -1)


def ring(block, axis, distance):
    size = lax.axis_size(axis)
    return lax.ppermute(block, axis, [(i, (i + distance) % size) for i in range(size)])


def swap(block, axis, which):
    size = lax.axis_size(axis)
    pairs = [(i, ((i + which) ^ 1) - which) for i in range(size)]
    return lax.ppermute(block, axis, [(i, j % size) for i, j in pairs])


def scalars():
    return pl.BlockSpec(memory_space=pltpu.SMEM)


def held():
    return pl.BlockSpec(memory_space=pltpu.VMEM)


def near(values):
    return pltpu.with_memory_space_constraint(values, pltpu.VMEM)


def array(*shape, dtype=jnp.float32):
    return pltpu.VMEM(shape, dtype)


def call(body, name, args, outs, flops=2_000_000, **extra):
    if "in_specs" not in extra:
        args = [near(arg) for arg in args]
        extra["in_specs"] = [held() for _ in args]
        extra["out_specs"] = tuple(held() for _ in outs) if isinstance(outs, tuple) else held()
    return pl.pallas_call(
        body,
        out_shape=outs,
        name=name,
        cost_estimate=pl.CostEstimate(flops=flops, transcendentals=0, bytes_accessed=500_000),
        **extra,
    )(*args)


def one_hot(cells, width):
    lower = (cells & (width - 1)).astype(jnp.float32).astype(jnp.bfloat16)
    index = lax.broadcasted_iota(jnp.int32, (width, PPT), 0).astype(jnp.float32)
    return jnp.where(index.astype(jnp.bfloat16) == lower, jnp.bfloat16(1), jnp.bfloat16(0))


def upper_index(cells, width, count):
    living = lax.broadcasted_iota(jnp.int32, (1, PPT), 1) < count
    return jnp.where(living, cells >> (width.bit_length() - 1), -1)


def store_deposits(off, vel, aff, mass, amounts, begin=0, rows=8):
    span = slice(begin, begin + rows)
    masses = mass[span, :]
    amounts[0, span, :] = masses.astype(jnp.bfloat16).astype(jnp.float32)
    for a in range(3):
        affine = [aff[3 * a + e, span, :] * off[e, span, :] for e in range(3)]
        drift = vel[a, span, :] - (affine[0] + affine[1] + affine[2])
        amounts[a + 1, span, :] = (masses * drift).astype(jnp.bfloat16).astype(jnp.float32)


def splat_row(cell, amounts, row, count):
    half = LANES // 2
    cells = cell[row : row + 1, :]
    upper = upper_index(cells, half, count)
    position = lax.broadcasted_iota(jnp.int32, (8, PPT), 0)
    chosen = [
        jnp.where(
            position < UPPER,
            amounts[2 * pair, row : row + 1, :],
            amounts[2 * pair + 1, row : row + 1, :],
        )
        for pair in range(2)
    ]
    weighted = []
    for side in range(2):
        there = 2 * (position & (UPPER - 1)) + side == upper
        weighted += [jnp.where(there, values, 0.0) for values in chosen]
    summed = lax.dot_general(
        jnp.concatenate(weighted, axis=0).astype(jnp.bfloat16),
        one_hot(cells, half),
        (((1,), (1,)), ((), ())),
        preferred_element_type=jnp.float32,
    )
    return jnp.concatenate([summed[:REC], summed[REC:]], axis=1)


def particle_specs(start):
    return [
        pl.BlockSpec((8, PPT), lambda i: (i + start, 0)),
        pl.BlockSpec((3, 8, PPT), lambda i: (0, i + start, 0)),
        pl.BlockSpec((3, 8, PPT), lambda i: (0, i + start, 0)),
        pl.BlockSpec((9, 8, PPT), lambda i: (0, i + start, 0)),
        pl.BlockSpec((8, PPT), lambda i: (i + start, 0)),
    ]


def splat_own(counts, slots, parts, start, blocks):
    def body(counts, slots, cell, off, vel, aff, mass, acc, amounts):
        @pl.when(pl.program_id(0) == 0)
        def _():
            acc[...] = jnp.zeros_like(acc)

        store_deposits(off, vel, aff, mass, amounts)
        base = (pl.program_id(0) + start) * 8
        summed = [splat_row(cell, amounts, row, counts[base + row]) for row in range(8)]
        for row in range(8):
            place = pl.multiple_of(slots[base + row] * REC, REC)
            acc[pl.ds(place, REC), :] += summed[row]

    return call(
        body,
        "splat_own",
        (counts, slots, *parts),
        array(TPD * REC, LANES),
        flops=blocks * 8 * 2_000_000,
        grid=(blocks,),
        in_specs=[scalars(), scalars()] + particle_specs(start),
        out_specs=held(),
        scratch_shapes=[pltpu.VMEM((4, 8, PPT), jnp.float32)],
    )


FIRST = OWN_BINS // 8
block_rows = (8, 8, 8, 2)
side_rows = (tuple(range(8)), (0,), tuple(range(1, 8)), (0, 1))
middle_rows = {1: tuple(range(1, 8)), 2: (0,)}


def side_place(number):
    return (0, number) if number < GROUP else (1, number - 17)


def splat_sides(tile_coords, owner_map, bin_tile, counts, parts):
    def body(coords, owner_map, bin_tile, counts, *rest):
        sources, rest = rest[:5], rest[5:]
        slots, code_row, code_column, slot_rows, below, above = rest[:6]
        near_parts, amounts, owners, arrived, listed = rest[6:11], *rest[11:]
        fetch = pltpu.make_async_copy(owner_map, owners, listed)
        fetch.start()
        waits = []
        for block, rows in enumerate(block_rows):
            waits.append([])
            for n, (source, target) in enumerate(zip(sources, near_parts)):
                taken = (slice(None),) * (len(source.shape) - 2)
                copy = pltpu.make_async_copy(
                    source.at[(*taken, pl.ds(OWN_BINS + 8 * block, rows))],
                    target.at[(*taken, pl.ds(8 * block, rows))],
                    arrived.at[block, n],
                )
                waits[block].append(copy)

        def prepare():
            fetch.wait()
            for number in range(BINS):
                slots[number] = owners[bin_tile[number]] & (TPD - 1)
            for number in range(NBR_BINS):
                value = slots[OWN_BINS + number].astype(jnp.float32)
                slot_rows[number : number + 1, :] = jnp.full((1, LANES), value, jnp.float32)
            turn_of = lax.broadcasted_iota(jnp.int32, (8, LANES), 1) & (TPD - 1)
            row_of = lax.broadcasted_iota(jnp.int32, (TPD, LANES), 0)
            along, down = jnp.zeros((8, LANES), jnp.int32), jnp.zeros((TPD, LANES), jnp.int32)
            for t in range(TPD):
                code = (coords[0, t] + 1) * 4096 + (coords[1, t] + 1) * 64 + coords[2, t] + 1
                along = jnp.where(turn_of == t, code, along)
                down = jnp.where(row_of == t, code, down)
            code_row[...] = along.astype(jnp.float32)
            code_column[...] = down.astype(jnp.float32)
            for out, begin in ((below, 0), (above, 17)):
                out[META : META + GROUP, :] = slot_rows[begin : begin + GROUP, :]
                out[META + GROUP : META + GROUP + 1, :] = code_row[0:1, :]
                out[META + GROUP + 1 : PAYLOAD, :] = jnp.zeros((6, LANES), jnp.float32)

        for block in (0, 1):
            for copy in waits[block]:
                copy.start()
        for block, rows in enumerate(block_rows):
            for copy in waits[block]:
                copy.wait()
            if block == 0:
                for copy in waits[2] + waits[3]:
                    copy.start()
            if block == 1:
                prepare()
            cell, off, vel, aff, mass = near_parts
            store_deposits(off, vel, aff, mass, amounts, 8 * block, rows)
            for row in side_rows[block]:
                number = block * 8 + row
                way, index = side_place(number)
                out = (below, above)[way]
                out[index * REC : (index + 1) * REC, :] = splat_row(
                    cell, amounts, number, counts[OWN_BINS + number]
                )

    return call(
        body,
        "splat_sides",
        (tile_coords, owner_map, bin_tile, counts, *parts),
        (
            pltpu.SMEM((BINS,), jnp.int32),
            array(8, LANES),
            array(TPD, LANES),
            array(32, LANES),
            array(PAYLOAD, LANES),
            array(PAYLOAD, LANES),
        ),
        flops=18 * 2_000_000,
        in_specs=[scalars(), pl.BlockSpec(memory_space=pl.ANY), scalars(), scalars()]
        + [pl.BlockSpec(memory_space=pl.ANY)] * 5,
        out_specs=(scalars(),) + (held(),) * 5,
        scratch_shapes=[
            pltpu.VMEM((32, PPT), jnp.int32),
            pltpu.VMEM((3, 32, PPT), jnp.float32),
            pltpu.VMEM((3, 32, PPT), jnp.float32),
            pltpu.VMEM((9, 32, PPT), jnp.float32),
            pltpu.VMEM((32, PPT), jnp.float32),
            pltpu.VMEM((4, 32, PPT), jnp.float32),
            pltpu.SMEM((OWNERS,), jnp.int32),
            pltpu.SemaphoreType.DMA((4, 5)),
            pltpu.SemaphoreType.DMA,
        ],
    )


def splat_middle(counts, slots, parts):
    def body(counts, slots, cell, off, vel, aff, mass, middle, amounts):
        store_deposits(off, vel, aff, mass, amounts)

        def splat(block, rows):
            @pl.when(pl.program_id(0) == block - 1)
            def _():
                for row in rows:
                    number = block * 8 + row
                    index = number - GROUP
                    middle[index * REC : (index + 1) * REC, :] = splat_row(
                        cell, amounts, row, counts[OWN_BINS + number]
                    )

        for block, rows in middle_rows.items():
            splat(block, rows)

    return call(
        body,
        "splat_middle",
        (counts, slots, *parts),
        array(8 * REC, LANES),
        flops=8 * 2_000_000,
        grid=(2,),
        in_specs=[scalars(), scalars()] + particle_specs(FIRST + 1),
        out_specs=held(),
        scratch_shapes=[pltpu.VMEM((4, 8, PPT), jnp.float32)],
    )


middle_steps = [(b, c) for b in (-1, 0, 1) for c in (-1, 0, 1) if (b, c) != (0, 0)]


def mid_of(dy, dz):
    return ("mid", middle_steps.index((dy, dz)))


def y_sources(orient):
    listing = [mid_of(orient, dz) for dz in (-1, 0, 1)]
    for arrived in ("xp", "xm"):
        listing += [(arrived, (orient + 1) * 3 + dz + 1) for dz in (-1, 0, 1)]
    return listing


def z_sources(orient):
    listing = [mid_of(0, orient)]
    listing += [(arrived, 3 + orient + 1) for arrived in ("xp", "xm")]
    for arrived in ("yp", "ym"):
        listing += [(arrived, 3 * group + orient + 1) for group in range(3)]
    return listing


consumed = (
    [("zp", n) for n in range(9)]
    + [("zm", n) for n in range(9)]
    + [("yp", 3 * g + 1) for g in range(3)]
    + [("ym", 3 * g + 1) for g in range(3)]
    + [("xp", 4), ("xm", 4)]
)


def y_reply_sources(sign):
    local, offset = (18, 3) if sign > 0 else (21, 6)
    listing = []
    for g in range(3):
        listing += [("zm", offset + g), ("rec", local + g), ("zp", offset + g)]
    return listing


def x_reply_sources(sign):
    group = 1 if sign > 0 else 2
    local = ("rec", 24 if sign > 0 else 25)
    return (
        [("ym", 3 * group + n) for n in range(3)]
        + [("zm", group), local, ("zp", group)]
        + [("yp", 3 * group + n) for n in range(3)]
    )


final_sources = (
    [("xm", n) for n in range(9)]
    + [("ym", n) for n in range(3)]
    + [("zm", 0), ("zp", 0)]
    + [("yp", n) for n in range(3)]
    + [("xp", n) for n in range(9)]
)


def record(ref, number):
    return ref[number * REC : (number + 1) * REC, :]


def slot_row(refs, source, slot_rows):
    name, number = source
    if name == "mid":
        return slot_rows[GROUP + number : GROUP + number + 1, :]
    return refs[name][META + number : META + number + 1, :]


def forward(names, buffers, slot_rows, code_row, sources, title):
    def body(*refs):
        kept = dict(zip(names, refs))
        slots, codes = refs[len(names)], refs[len(names) + 1]
        for out, listing in zip(refs[len(names) + 2 :], sources):
            for number, source in enumerate(listing):
                out[number * REC : (number + 1) * REC, :] = record(kept[source[0]], source[1])
                out[META + number : META + number + 1, :] = slot_row(kept, source, slots)
            out[META + GROUP : META + GROUP + 1, :] = codes[0:1, :]
            out[META + GROUP + 1 : PAYLOAD, :] = jnp.zeros((6, LANES), jnp.float32)

    payload = array(PAYLOAD, LANES)
    return call(body, title, (*buffers, slot_rows, code_row), (payload, payload))


def reply(names, buffers, sources, title):
    def body(*refs):
        kept = dict(zip(names, refs))
        for out, listing in zip(refs[len(names) :], sources):
            for number, source in enumerate(listing):
                out[number * REC : (number + 1) * REC, :] = record(kept[source[0]], source[1])

    payload = array(META, LANES)
    return call(body, title, tuple(buffers), (payload, payload))


def thirds(values):
    high = values.astype(jnp.bfloat16)
    rest = values - high.astype(jnp.float32)
    middle = rest.astype(jnp.bfloat16)
    low = (rest - middle.astype(jnp.float32)).astype(jnp.bfloat16)
    return high, middle, low


def pick(hot, values):
    found = None
    for part in thirds(values):
        term = lax.dot_general(
            hot, part, (((1,), (0,)), ((), ())), preferred_element_type=jnp.float32
        )
        found = term if found is None else found + term
    return found


def cell_axes():
    lane = lax.broadcasted_iota(jnp.int32, (TPD, CELLS), 1)
    return lane >> 6, (lane >> 3) & 7, lane & 7


def turn(values, shift):
    return pltpu.roll(values, shift % CELLS, 1)


def beside(values, ghost, facing):
    axis, step = facing // 2, (64, 8, 1)[facing // 2]
    index = cell_axes()[axis]
    if facing % 2 == 0:
        return jnp.where(index == 7, turn(ghost, 7 * step), turn(values, -step))
    return jnp.where(index == 0, turn(ghost, -7 * step), turn(values, step))


def table_of(refs):
    width = refs[0].shape[1]
    rows = [ref[...] for ref in refs]
    return jnp.concatenate(rows + [jnp.zeros((LANES - 7 * TPD, width), jnp.float32)], axis=0)


def ghosts_of(hot, refs):
    found = pick(hot, table_of(refs))
    return [found[TPD * facing : TPD * (facing + 1)] for facing in range(6)]


def quarter(values, number):
    return values[:, number * LANES : (number + 1) * LANES]


def edge_lanes(rows):
    lane = lax.broadcasted_iota(jnp.int32, (rows, LANES), 1)
    z_face = ((lane + 1) & 7) < 2
    return z_face, z_face & (((lane + 8) & 63) < 16)


def pack_faces(speeds):
    z_face, corner = edge_lanes(TPD)
    mixed, corners = [], None
    for number in range(4):
        uy, uz = quarter(speeds[1], number), quarter(speeds[2], number)
        mixed.append(jnp.where(z_face, uz, uy))
        turned = pltpu.roll(jnp.where(corner, uy, 0.0), 2 * number, 1)
        corners = turned if corners is None else corners + turned
    low = lax.broadcasted_iota(jnp.int32, (TPD, LANES), 1) < 64
    sides = jnp.where(low, quarter(speeds[0], 0), quarter(speeds[0], 3))
    return jnp.concatenate(mixed + [corners, sides], axis=1)


def face_ghost(found, facing):
    if facing < 2:
        sides = found[:, CELLS + LANES : FACES]
        return jnp.concatenate([sides] * 4, axis=1)
    if facing > 3:
        return found[:, :CELLS]
    corners = found[:, CELLS : CELLS + LANES]
    z_face, _ = edge_lanes(TPD)
    return jnp.concatenate(
        [
            jnp.where(
                z_face, pltpu.roll(corners, (LANES - 2 * n) % LANES, 1), quarter(found, n)
            )
            for n in range(4)
        ],
        axis=1,
    )


def gather_grid(arrivals, accs):
    names = ("xp", "xm", "yp", "ym", "zp", "zm")

    def body(*refs):
        kept = dict(zip(names, refs[:6]))
        own = refs[6 : 6 + len(accs)]
        velocity, faces, fluid_out, slots_out, rec = refs[6 + len(accs) :]
        for number, source in enumerate(consumed):
            rec[number * REC : (number + 1) * REC, :] = record(kept[source[0]], source[1])
            slots_out[number : number + 1, :] = slot_row(kept, source, None)
        rec[NBR_BINS * REC : 32 * REC, :] = jnp.zeros(((32 - NBR_BINS) * REC, LANES), jnp.float32)
        slots_out[NBR_BINS:32, :] = jnp.full((32 - NBR_BINS, LANES), -1.0, jnp.float32)
        hot = (
            slots_out[...] == lax.broadcasted_iota(jnp.int32, (32, LANES), 1).astype(jnp.float32)
        ).astype(jnp.float32)
        hot = jnp.transpose(hot)[:TPD, :].astype(jnp.bfloat16)
        received = jnp.concatenate([rec[pl.ds(r, 32, stride=REC), :] for r in range(REC)], axis=1)
        totals = pick(hot, received)
        for acc in own:
            totals = totals + jnp.concatenate(
                [acc[pl.ds(r, TPD, stride=REC), :] for r in range(REC)], axis=1
            )
        masses = totals[:, :CELLS]
        fluid = masses > 0.0
        safe = jnp.where(fluid, masses, 1.0)
        speeds = []
        for a in range(3):
            value = totals[:, (a + 1) * CELLS : (a + 2) * CELLS] / safe
            if a == 1:
                value = value - 0.5
            speeds.append(jnp.where(fluid, value, 0.0))
            velocity[:, a * CELLS : (a + 1) * CELLS] = speeds[a]
        faces[...] = pack_faces(speeds)
        fluid_out[...] = fluid.astype(jnp.float32)

    return call(
        body,
        "gather_grid",
        (*arrivals, *accs),
        (
            array(TPD, 3 * CELLS),
            array(TPD, FACES),
            array(TPD, CELLS),
            array(32, LANES),
        ),
        scratch_shapes=[pltpu.VMEM((32 * REC, LANES), jnp.float32)],
    )


def divergence(arrivals, code_row, code_column, velocity, faces, fluid, arrived):
    def body(*refs):
        payloads, code_row, code_column, fluid, velocity = refs[:6], *refs[6:10]
        fields = refs[10:17]
        hot_out, div_out, pressure = refs[17:]
        group = lax.broadcasted_iota(jnp.int32, (1, LANES), 1) // TPD
        codes = jnp.where(group == 0, code_row[0:1, :], -9999.0)
        for number, ref in enumerate(payloads):
            axis = number // 2
            which = (number + lax.axis_index(AXES[axis]) + 1) & 1
            slot = 1 + 3 * which + 2 - axis
            codes = jnp.where(group == slot, ref[META + GROUP : META + GROUP + 1, :], codes)
        hots = [
            (code_column[...] + float(step) == codes).astype(jnp.bfloat16) for step in face_codes
        ]
        hot = jnp.concatenate(hots, axis=0)
        hot_out[...] = hot
        total = None
        ghosts = [face_ghost(found, n) for n, found in enumerate(ghosts_of(hot, fields))]
        for a in range(3):
            own = velocity[:, a * CELLS : (a + 1) * CELLS]
            ahead, behind = ghosts[2 * a], ghosts[2 * a + 1]
            term = 0.5 * (beside(own, ahead, 2 * a) - beside(own, behind, 2 * a + 1))
            total = term if total is None else total + term
        div_out[...] = total
        pressure[...] = jnp.where(fluid[...] > 0.0, (0.0 - total) / 6.0, 0.0)

    field = array(TPD, CELLS)
    return call(
        body,
        "divergence",
        (*arrivals, code_row, code_column, fluid, velocity, faces, *arrived),
        (array(6 * TPD, LANES, dtype=jnp.bfloat16), field, field),
    )


def sweep(hot, div, fluid, pressure, arrived):
    def body(hot, div, fluid, *refs):
        fields, out = refs[:7], refs[7]
        values = fields[0][...]
        total = None
        for facing, ghost in enumerate(ghosts_of(hot[...], fields)):
            term = beside(values, ghost, facing)
            total = term if total is None else total + term
        out[...] = jnp.where(fluid[...] > 0.0, (total - div[...]) / 6.0, 0.0)

    return call(
        body,
        "sweep",
        (hot, div, fluid, pressure, *arrived),
        array(TPD, CELLS),
    )


def project(hot, fluid, velocity, slots, pressure, arrived):
    def body(hot, fluid, velocity, slots, *refs):
        fields = refs[:7]
        tiles, back_p, back_m, back_local, rec = refs[7:]
        values = fields[0][...]
        ghosts = ghosts_of(hot[...], fields)
        wet = fluid[...] > 0.0
        tiles[...] = jnp.zeros_like(tiles)
        rec[...] = jnp.zeros_like(rec)
        named = (
            slots[...] == lax.broadcasted_iota(jnp.int32, (32, LANES), 1).astype(jnp.float32)
        ).astype(jnp.bfloat16)[:, :TPD]
        for a in range(3):
            slope = 0.5 * (
                beside(values, ghosts[2 * a], 2 * a) - beside(values, ghosts[2 * a + 1], 2 * a + 1)
            )
            final = jnp.where(wet, velocity[:, a * CELLS : (a + 1) * CELLS] - slope, 0.0)
            copies = pick(named, final)
            for u in range(UPPER):
                row = a * UPPER + u
                tiles[pl.ds(row, TPD, stride=REC), :] = final[:, u * LANES : (u + 1) * LANES]
                rec[pl.ds(row, 32, stride=REC), :] = copies[:, u * LANES : (u + 1) * LANES]
        back_p[...] = rec[:META, :]
        back_m[...] = rec[META : 2 * META, :]
        back_local[...] = rec[2 * META : NBR_BINS * REC, :]

    block = array(META, LANES)
    return call(
        body,
        "project",
        (hot, fluid, velocity, slots, pressure, *arrived),
        (
            array(TPD * REC, LANES),
            block,
            block,
            array(8 * REC, LANES),
        ),
        scratch_shapes=[pltpu.VMEM((32 * REC, LANES), jnp.float32)],
    )


def results(tiles, pressure):
    def body(tiles, pressure, grid_out, pressure_out):
        for t in range(TPD):
            for u in range(UPPER):
                begin = t * CELLS + u * LANES
                grid_out[:, begin : begin + LANES] = tiles[pl.ds(t * REC + u, 3, stride=UPPER), :]
        for u in range(UPPER):
            pressure_out[pl.ds(u, TPD, stride=UPPER), :] = pressure[:, u * LANES : (u + 1) * LANES]

    return call(
        body,
        "results",
        (tiles, pressure),
        (array(3, TPD * CELLS), array(TPD * UPPER, LANES)),
    )


def sample_row(cell, tile, row, count):
    cells = cell[row : row + 1, :]
    upper = upper_index(cells, LANES, count)
    high = tile.astype(jnp.bfloat16)
    low = (tile - high.astype(jnp.float32)).astype(jnp.bfloat16)
    planes = lax.dot_general(
        jnp.concatenate([high, low], axis=0),
        one_hot(cells, LANES),
        (((1,), (0,)), ((), ())),
        preferred_element_type=jnp.float32,
    )
    planes = planes[:REC] + planes[REC:]
    wanted = (lax.broadcasted_iota(jnp.int32, (8, PPT), 0) & (UPPER - 1)) == upper
    sums = []
    for half in range(2):
        kept = jnp.where(wanted, planes[8 * half : 8 * half + 8], 0.0)
        kept = kept + pltpu.roll(kept, 7, 0)
        sums.append(kept + pltpu.roll(kept, 6, 0))
    return sums[0][0:1], sums[0][4:5], sums[1][0:1]


def store_row(out, row, values):
    for a in range(3):
        out[a, row : row + 1, :] = values[a]


particle_shape = jax.ShapeDtypeStruct((3, BINS, PPT), jnp.float32)


def sample_own(counts, slots, cell, tiles, sampled, start, blocks):
    def body(counts, slots, cell, tiles, *refs):
        out = refs[-1]
        base = (pl.program_id(0) + start) * 8
        for row in range(8):
            place = pl.multiple_of(slots[base + row] * REC, REC)
            tile = tiles[pl.ds(place, REC), :]
            store_row(out, row, sample_row(cell, tile, row, counts[base + row]))

    args = [counts, slots, cell, near(tiles)]
    specs = [
        scalars(),
        scalars(),
        pl.BlockSpec((8, PPT), lambda i: (i + start, 0)),
        held(),
    ]
    alias = {}
    if sampled is not None:
        args.append(sampled)
        specs.append(pl.BlockSpec(memory_space=pl.ANY))
        alias = {4: 0}
    return call(
        body,
        "sample_own",
        tuple(args),
        particle_shape,
        flops=blocks * 8 * 2_000_000,
        grid=(blocks,),
        in_specs=specs,
        out_specs=pl.BlockSpec((3, 8, PPT), lambda i: (0, i + start, 0)),
        input_output_aliases=alias,
    )


def sample_middle(counts, cell, buffers):
    names = ("yp", "ym", "zp", "zm")

    def body(counts, cell, *refs):
        held_by = dict(zip(names, refs))
        out = refs[len(names)]
        for block, rows in middle_rows.items():
            for row in rows:
                number = block * 8 + row
                name, index = final_sources[number]
                tile = record(held_by[name], index)
                values = sample_row(cell, tile, number, counts[OWN_BINS + number])
                store_row(out, number - GROUP, values)

    return call(
        body,
        "sample_middle",
        (counts, near(cell), *[near(buffer) for buffer in buffers]),
        array(3, 8, PPT),
        flops=8 * 2_000_000,
        in_specs=[scalars()] + [held()] * (1 + len(names)),
        out_specs=held(),
    )


def sample_sides(counts, cell, buffers, middle, sampled):
    def body(counts, cell, xp, xm, middle, sampled, out, buffer, sent):
        held_by = {"xp": xp, "xm": xm}
        copies = []
        for block in (0, 2, 1, 3):
            for row in side_rows[block]:
                number = block * 8 + row
                name, index = final_sources[number]
                tile = record(held_by[name], index)
                store_row(
                    buffer, number, sample_row(cell, tile, number, counts[OWN_BINS + number])
                )
            for row in middle_rows.get(block, ()):
                number = block * 8 + row
                index = number - GROUP
                store_row(buffer, number, [middle[a, index : index + 1, :] for a in range(3)])
            copy = pltpu.make_async_copy(
                buffer.at[:, pl.ds(8 * block, block_rows[block])],
                out.at[:, pl.ds(OWN_BINS + 8 * block, block_rows[block])],
                sent.at[block],
            )
            copy.start()
            copies.append(copy)
        for copy in copies:
            copy.wait()

    return call(
        body,
        "sample_sides",
        (counts, *[near(value) for value in (cell, *buffers, middle)], sampled),
        particle_shape,
        flops=18 * 2_000_000,
        in_specs=[scalars()] + [held()] * 4 + [pl.BlockSpec(memory_space=pl.ANY)],
        out_specs=pl.BlockSpec(memory_space=pl.ANY),
        input_output_aliases={5: 0},
        scratch_shapes=[pltpu.VMEM((3, 32, PPT), jnp.float32), pltpu.SemaphoreType.DMA((4,))],
    )


def exchange(values):
    return [swap(values, axis, which) for which in (0, 1) for axis in reversed(AXES)]


def together(*values):
    return lax.optimization_barrier(values)


def with_kept(sources):
    return [("kept", n - 18) if name == "rec" else (name, n) for name, n in sources]


def local(tile_coords, owner_map, bin_tile, counts, cell, offset, velocity, affine, mass):
    parts = (
        cell,
        jnp.transpose(offset, (1, 0, 2)),
        jnp.transpose(velocity, (1, 0, 2)),
        jnp.transpose(affine, (1, 0, 2)),
        mass,
    )
    slots, code_row, code_column, slot_rows, below, above = splat_sides(
        tile_coords, owner_map, bin_tile, counts, parts
    )
    xp, xm = ring(above, "gx", 1), ring(below, "gx", -1)
    middle = splat_middle(counts, slots, parts)
    up, down = forward(
        ("mid", "xp", "xm"),
        (middle, xp, xm),
        slot_rows,
        code_row,
        (y_sources(1), y_sources(-1)),
        "forward_y",
    )
    slots, up, down = together(slots, up, down)
    yp, ym = ring(up, "gy", 1), ring(down, "gy", -1)
    acc_y = splat_own(counts, slots, parts, 0, 2)
    yp, ym, acc_y = together(yp, ym, acc_y)
    up, down = forward(
        ("mid", "xp", "xm", "yp", "ym"),
        (middle, xp, xm, yp, ym),
        slot_rows,
        code_row,
        (z_sources(1), z_sources(-1)),
        "forward_z",
    )
    slots, up, down = together(slots, up, down)
    zp, zm = ring(up, "gz", 1), ring(down, "gz", -1)
    acc_z = splat_own(counts, slots, parts, 2, 2)
    arrivals = (xp, xm, yp, ym, zp, zm)
    grid_u, faces, fluid, nbr_slots = gather_grid(arrivals, (acc_y, acc_z))
    hot, div, pressure = divergence(
        arrivals, code_row, code_column, grid_u, faces, fluid, exchange(faces)
    )
    for _ in range(SWEEPS - 1):
        pressure = sweep(hot, div, fluid, pressure, exchange(pressure))
    leaving = lax.slice_in_dim(together(cell, div)[0], OWN_BINS, BINS, axis=0)
    tiles, back_p, back_m, kept = project(
        hot, fluid, grid_u, nbr_slots, pressure, exchange(pressure)
    )
    rzp, rzm = ring(back_p, "gz", -1), ring(back_m, "gz", 1)
    sampled = sample_own(counts, slots, cell, tiles, None, 0, 2)
    rzp, rzm, sampled = together(rzp, rzm, sampled)
    up, down = reply(
        ("kept", "zp", "zm"),
        (kept, rzp, rzm),
        (with_kept(y_reply_sources(1)), with_kept(y_reply_sources(-1))),
        "reply_y",
    )
    slots, up, down = together(slots, up, down)
    ryp, rym = ring(up, "gy", -1), ring(down, "gy", 1)
    sampled = sample_own(counts, slots, cell, tiles, sampled, 2, 2)
    ryp, rym, sampled = together(ryp, rym, sampled)
    up, down = reply(
        ("kept", "zp", "zm", "yp", "ym"),
        (kept, rzp, rzm, ryp, rym),
        (with_kept(x_reply_sources(1)), with_kept(x_reply_sources(-1))),
        "reply_x",
    )
    slots, up, down = together(slots, up, down)
    rxp, rxm = ring(up, "gx", -1), ring(down, "gx", 1)
    middle = sample_middle(counts, leaving, (ryp, rym, rzp, rzm))
    grid_v, final_pressure = results(tiles, pressure)
    sampled = sample_sides(counts, leaving, (rxp, rxm), middle, sampled)
    return grid_v, final_pressure.reshape(-1), jnp.transpose(sampled, (1, 0, 2))


def solution(mesh):
    split = P(AXES)
    particles = P(AXES, None, None)
    return jax.shard_map(
        local,
        mesh=mesh,
        in_specs=(
            P(None, AXES),
            P(),
            split,
            split,
            P(AXES, None),
            particles,
            particles,
            particles,
            P(AXES, None),
        ),
        out_specs=(P(None, AXES), split, particles),
        check_vma=False,
    )
```

```python
import jax
import jax.numpy as jnp
from jax import lax
from jax.experimental import pallas as pl
from jax.experimental.pallas import tpu as pltpu
from jax.sharding import PartitionSpec as P

TPD = 16
OWN_BINS = 32
NBR_BINS = 26
BINS = OWN_BINS + NBR_BINS
PPT = 2048
CELLS = 512
LANES = 128
UPPER = CELLS // LANES
REC = 16
GROUP = 9
META = GROUP * REC
PAYLOAD = META + 16
SWEEPS = 4
AXES = ("gx", "gy", "gz")
OWNERS = 4096
FACES = CELLS + 2 * LANES
face_codes = (4096, -4096, 64, -64, 1, -1)


def ring(block, axis, distance):
    size = lax.axis_size(axis)
    return lax.ppermute(block, axis, [(i, (i + distance) % size) for i in range(size)])


def swap(block, axis, which):
    size = lax.axis_size(axis)
    pairs = [(i, ((i + which) ^ 1) - which) for i in range(size)]
    return lax.ppermute(block, axis, [(i, j % size) for i, j in pairs])


def scalars():
    return pl.BlockSpec(memory_space=pltpu.SMEM)


def held():
    return pl.BlockSpec(memory_space=pltpu.VMEM)


def near(values):
    return pltpu.with_memory_space_constraint(values, pltpu.VMEM)


def array(*shape, dtype=jnp.float32):
    return pltpu.VMEM(shape, dtype)


def call(body, name, args, outs, flops=2_000_000, **extra):
    if "in_specs" not in extra:
        args = [near(arg) for arg in args]
        extra["in_specs"] = [held() for _ in args]
        extra["out_specs"] = tuple(held() for _ in outs) if isinstance(outs, tuple) else held()
    return pl.pallas_call(
        body,
        out_shape=outs,
        name=name,
        cost_estimate=pl.CostEstimate(flops=flops, transcendentals=0, bytes_accessed=500_000),
        **extra,
    )(*args)


def one_hot(cells, width):
    lower = (cells & (width - 1)).astype(jnp.float32).astype(jnp.bfloat16)
    index = lax.broadcasted_iota(jnp.int32, (width, PPT), 0).astype(jnp.float32)
    return jnp.where(index.astype(jnp.bfloat16) == lower, jnp.bfloat16(1), jnp.bfloat16(0))


def upper_index(cells, width, count):
    living = lax.broadcasted_iota(jnp.int32, (1, PPT), 1) < count
    return jnp.where(living, cells >> (width.bit_length() - 1), -1)


def store_deposits(off, vel, aff, mass, amounts, begin=0, rows=8):
    span = slice(begin, begin + rows)
    masses = mass[span, :]
    amounts[0, span, :] = masses.astype(jnp.bfloat16).astype(jnp.float32)
    for a in range(3):
        affine = [aff[3 * a + e, span, :] * off[e, span, :] for e in range(3)]
        drift = vel[a, span, :] - (affine[0] + affine[1] + affine[2])
        amounts[a + 1, span, :] = (masses * drift).astype(jnp.bfloat16).astype(jnp.float32)


def splat_row(cell, amounts, row, count):
    half = LANES // 2
    cells = cell[row : row + 1, :]
    upper = upper_index(cells, half, count)
    position = lax.broadcasted_iota(jnp.int32, (8, PPT), 0)
    chosen = [
        jnp.where(
            position < UPPER,
            amounts[2 * pair, row : row + 1, :],
            amounts[2 * pair + 1, row : row + 1, :],
        )
        for pair in range(2)
    ]
    weighted = []
    for side in range(2):
        there = 2 * (position & (UPPER - 1)) + side == upper
        weighted += [jnp.where(there, values, 0.0) for values in chosen]
    summed = lax.dot_general(
        jnp.concatenate(weighted, axis=0).astype(jnp.bfloat16),
        one_hot(cells, half),
        (((1,), (1,)), ((), ())),
        preferred_element_type=jnp.float32,
    )
    return jnp.concatenate([summed[:REC], summed[REC:]], axis=1)


def particle_specs(start):
    return [
        pl.BlockSpec((8, PPT), lambda i: (i + start, 0)),
        pl.BlockSpec((3, 8, PPT), lambda i: (0, i + start, 0)),
        pl.BlockSpec((3, 8, PPT), lambda i: (0, i + start, 0)),
        pl.BlockSpec((9, 8, PPT), lambda i: (0, i + start, 0)),
        pl.BlockSpec((8, PPT), lambda i: (i + start, 0)),
    ]


def splat_own(counts, slots, parts, start, blocks):
    def body(counts, slots, cell, off, vel, aff, mass, acc, amounts):
        @pl.when(pl.program_id(0) == 0)
        def _():
            acc[...] = jnp.zeros_like(acc)

        store_deposits(off, vel, aff, mass, amounts)
        base = (pl.program_id(0) + start) * 8
        summed = [splat_row(cell, amounts, row, counts[base + row]) for row in range(8)]
        for row in range(8):
            place = pl.multiple_of(slots[base + row] * REC, REC)
            acc[pl.ds(place, REC), :] += summed[row]

    return call(
        body,
        "splat_own",
        (counts, slots, *parts),
        array(TPD * REC, LANES),
        flops=blocks * 8 * 2_000_000,
        grid=(blocks,),
        in_specs=[scalars(), scalars()] + particle_specs(start),
        out_specs=held(),
        scratch_shapes=[pltpu.VMEM((4, 8, PPT), jnp.float32)],
    )


FIRST = OWN_BINS // 8
block_rows = (8, 8, 8, 2)
side_rows = (tuple(range(8)), (0,), tuple(range(1, 8)), (0, 1))
middle_rows = {1: tuple(range(1, 8)), 2: (0,)}


def side_place(number):
    return (0, number) if number < GROUP else (1, number - 17)


def splat_sides(tile_coords, owner_map, bin_tile, counts, parts):
    def body(*refs):
        tables, sources, rest = refs[:4], refs[4:9], refs[9:]
        slots, code_row, code_column, slot_rows, below, above = rest[:6]
        near_parts, amounts, arrived, listed = rest[6:11], rest[11], rest[12], rest[13]
        counts, coords, bin_tile, owners = rest[14:]
        fetches = [
            pltpu.make_async_copy(table, target, listed.at[n])
            for n, (table, target) in enumerate(zip(tables, rest[14:]))
        ]
        for fetch in fetches:
            fetch.start()
        waits = []
        for block, rows in enumerate(block_rows):
            waits.append([])
            for n, (source, target) in enumerate(zip(sources, near_parts)):
                taken = (slice(None),) * (len(source.shape) - 2)
                copy = pltpu.make_async_copy(
                    source.at[(*taken, pl.ds(OWN_BINS + 8 * block, rows))],
                    target.at[(*taken, pl.ds(8 * block, rows))],
                    arrived.at[block, n],
                )
                waits[block].append(copy)

        def prepare():
            for fetch in fetches[1:]:
                fetch.wait()
            for number in range(BINS):
                slots[number] = owners[bin_tile[number]] & (TPD - 1)
            for number in range(NBR_BINS):
                value = slots[OWN_BINS + number].astype(jnp.float32)
                slot_rows[number : number + 1, :] = jnp.full((1, LANES), value, jnp.float32)
            turn_of = lax.broadcasted_iota(jnp.int32, (8, LANES), 1) & (TPD - 1)
            row_of = lax.broadcasted_iota(jnp.int32, (TPD, LANES), 0)
            along, down = jnp.zeros((8, LANES), jnp.int32), jnp.zeros((TPD, LANES), jnp.int32)
            for t in range(TPD):
                code = (coords[0, t] + 1) * 4096 + (coords[1, t] + 1) * 64 + coords[2, t] + 1
                along = jnp.where(turn_of == t, code, along)
                down = jnp.where(row_of == t, code, down)
            code_row[...] = along.astype(jnp.float32)
            code_column[...] = down.astype(jnp.float32)
            for out, begin in ((below, 0), (above, 17)):
                out[META : META + GROUP, :] = slot_rows[begin : begin + GROUP, :]
                out[META + GROUP : META + GROUP + 1, :] = code_row[0:1, :]
                out[META + GROUP + 1 : PAYLOAD, :] = jnp.zeros((6, LANES), jnp.float32)

        for block in (0, 1):
            for copy in waits[block]:
                copy.start()
        fetches[0].wait()
        for block, rows in enumerate(block_rows):
            for copy in waits[block]:
                copy.wait()
            if block == 0:
                for copy in waits[2] + waits[3]:
                    copy.start()
            if block == 1:
                prepare()
            cell, off, vel, aff, mass = near_parts
            store_deposits(off, vel, aff, mass, amounts, 8 * block, rows)
            for row in side_rows[block]:
                number = block * 8 + row
                way, index = side_place(number)
                out = (below, above)[way]
                out[index * REC : (index + 1) * REC, :] = splat_row(
                    cell, amounts, number, counts[OWN_BINS + number]
                )

    return call(
        body,
        "splat_sides",
        (counts, tile_coords, bin_tile, owner_map, *parts),
        (
            pltpu.SMEM((BINS,), jnp.int32),
            array(8, LANES),
            array(TPD, LANES),
            array(32, LANES),
            array(PAYLOAD, LANES),
            array(PAYLOAD, LANES),
        ),
        flops=18 * 2_000_000,
        in_specs=[pl.BlockSpec(memory_space=pl.ANY)] * 9,
        out_specs=(scalars(),) + (held(),) * 5,
        scratch_shapes=[
            pltpu.VMEM((32, PPT), jnp.int32),
            pltpu.VMEM((3, 32, PPT), jnp.float32),
            pltpu.VMEM((3, 32, PPT), jnp.float32),
            pltpu.VMEM((9, 32, PPT), jnp.float32),
            pltpu.VMEM((32, PPT), jnp.float32),
            pltpu.VMEM((4, 32, PPT), jnp.float32),
            pltpu.SemaphoreType.DMA((4, 5)),
            pltpu.SemaphoreType.DMA((4,)),
            pltpu.SMEM((BINS,), jnp.int32),
            pltpu.SMEM((3, TPD), jnp.int32),
            pltpu.SMEM((BINS,), jnp.int32),
            pltpu.SMEM((OWNERS,), jnp.int32),
        ],
    )


def splat_middle(counts, slots, parts):
    def body(counts, slots, cell, off, vel, aff, mass, middle, amounts):
        store_deposits(off, vel, aff, mass, amounts)

        def splat(block, rows):
            @pl.when(pl.program_id(0) == block - 1)
            def _():
                for row in rows:
                    number = block * 8 + row
                    index = number - GROUP
                    middle[index * REC : (index + 1) * REC, :] = splat_row(
                        cell, amounts, row, counts[OWN_BINS + number]
                    )

        for block, rows in middle_rows.items():
            splat(block, rows)

    return call(
        body,
        "splat_middle",
        (counts, slots, *parts),
        array(8 * REC, LANES),
        flops=8 * 2_000_000,
        grid=(2,),
        in_specs=[scalars(), scalars()] + particle_specs(FIRST + 1),
        out_specs=held(),
        scratch_shapes=[pltpu.VMEM((4, 8, PPT), jnp.float32)],
    )


middle_steps = [(b, c) for b in (-1, 0, 1) for c in (-1, 0, 1) if (b, c) != (0, 0)]


def mid_of(dy, dz):
    return ("mid", middle_steps.index((dy, dz)))


def y_sources(orient):
    listing = [mid_of(orient, dz) for dz in (-1, 0, 1)]
    for arrived in ("xp", "xm"):
        listing += [(arrived, (orient + 1) * 3 + dz + 1) for dz in (-1, 0, 1)]
    return listing


def z_sources(orient):
    listing = [mid_of(0, orient)]
    listing += [(arrived, 3 + orient + 1) for arrived in ("xp", "xm")]
    for arrived in ("yp", "ym"):
        listing += [(arrived, 3 * group + orient + 1) for group in range(3)]
    return listing


consumed = (
    [("zp", n) for n in range(9)]
    + [("zm", n) for n in range(9)]
    + [("yp", 3 * g + 1) for g in range(3)]
    + [("ym", 3 * g + 1) for g in range(3)]
    + [("xp", 4), ("xm", 4)]
)


def y_reply_sources(sign):
    local, offset = (18, 3) if sign > 0 else (21, 6)
    listing = []
    for g in range(3):
        listing += [("zm", offset + g), ("rec", local + g), ("zp", offset + g)]
    return listing


def x_reply_sources(sign):
    group = 1 if sign > 0 else 2
    local = ("rec", 24 if sign > 0 else 25)
    return (
        [("ym", 3 * group + n) for n in range(3)]
        + [("zm", group), local, ("zp", group)]
        + [("yp", 3 * group + n) for n in range(3)]
    )


final_sources = (
    [("xm", n) for n in range(9)]
    + [("ym", n) for n in range(3)]
    + [("zm", 0), ("zp", 0)]
    + [("yp", n) for n in range(3)]
    + [("xp", n) for n in range(9)]
)


def record(ref, number):
    return ref[number * REC : (number + 1) * REC, :]


def slot_row(refs, source, slot_rows):
    name, number = source
    if name == "mid":
        return slot_rows[GROUP + number : GROUP + number + 1, :]
    return refs[name][META + number : META + number + 1, :]


def forward(names, buffers, slot_rows, code_row, sources, title):
    def body(*refs):
        kept = dict(zip(names, refs))
        slots, codes = refs[len(names)], refs[len(names) + 1]
        for out, listing in zip(refs[len(names) + 2 :], sources):
            for number, source in enumerate(listing):
                out[number * REC : (number + 1) * REC, :] = record(kept[source[0]], source[1])
                out[META + number : META + number + 1, :] = slot_row(kept, source, slots)
            out[META + GROUP : META + GROUP + 1, :] = codes[0:1, :]
            out[META + GROUP + 1 : PAYLOAD, :] = jnp.zeros((6, LANES), jnp.float32)

    payload = array(PAYLOAD, LANES)
    return call(body, title, (*buffers, slot_rows, code_row), (payload, payload))


def reply(names, buffers, sources, title):
    def body(*refs):
        kept = dict(zip(names, refs))
        for out, listing in zip(refs[len(names) :], sources):
            for number, source in enumerate(listing):
                out[number * REC : (number + 1) * REC, :] = record(kept[source[0]], source[1])

    payload = array(META, LANES)
    return call(body, title, tuple(buffers), (payload, payload))


def thirds(values):
    high = values.astype(jnp.bfloat16)
    rest = values - high.astype(jnp.float32)
    middle = rest.astype(jnp.bfloat16)
    low = (rest - middle.astype(jnp.float32)).astype(jnp.bfloat16)
    return high, middle, low


def pick(hot, values):
    found = None
    for part in thirds(values):
        term = lax.dot_general(
            hot, part, (((1,), (0,)), ((), ())), preferred_element_type=jnp.float32
        )
        found = term if found is None else found + term
    return found


def cell_axes():
    lane = lax.broadcasted_iota(jnp.int32, (TPD, CELLS), 1)
    return lane >> 6, (lane >> 3) & 7, lane & 7


def turn(values, shift):
    return pltpu.roll(values, shift % CELLS, 1)


def beside(values, ghost, facing):
    axis, step = facing // 2, (64, 8, 1)[facing // 2]
    index = cell_axes()[axis]
    if facing % 2 == 0:
        return jnp.where(index == 7, turn(ghost, 7 * step), turn(values, -step))
    return jnp.where(index == 0, turn(ghost, -7 * step), turn(values, step))


def table_of(refs):
    width = refs[0].shape[1]
    rows = [ref[...] for ref in refs]
    return jnp.concatenate(rows + [jnp.zeros((LANES - 7 * TPD, width), jnp.float32)], axis=0)


def ghosts_of(hot, refs):
    found = pick(hot, table_of(refs))
    return [found[TPD * facing : TPD * (facing + 1)] for facing in range(6)]


def quarter(values, number):
    return values[:, number * LANES : (number + 1) * LANES]


def edge_lanes(rows):
    lane = lax.broadcasted_iota(jnp.int32, (rows, LANES), 1)
    z_face = ((lane + 1) & 7) < 2
    return z_face, z_face & (((lane + 8) & 63) < 16)


def pack_faces(speeds):
    z_face, corner = edge_lanes(TPD)
    mixed, corners = [], None
    for number in range(4):
        uy, uz = quarter(speeds[1], number), quarter(speeds[2], number)
        mixed.append(jnp.where(z_face, uz, uy))
        turned = pltpu.roll(jnp.where(corner, uy, 0.0), 2 * number, 1)
        corners = turned if corners is None else corners + turned
    low = lax.broadcasted_iota(jnp.int32, (TPD, LANES), 1) < 64
    sides = jnp.where(low, quarter(speeds[0], 0), quarter(speeds[0], 3))
    return jnp.concatenate(mixed + [corners, sides], axis=1)


def face_ghost(found, facing):
    if facing < 2:
        sides = found[:, CELLS + LANES : FACES]
        return jnp.concatenate([sides] * 4, axis=1)
    if facing > 3:
        return found[:, :CELLS]
    corners = found[:, CELLS : CELLS + LANES]
    z_face, _ = edge_lanes(TPD)
    return jnp.concatenate(
        [
            jnp.where(
                z_face, pltpu.roll(corners, (LANES - 2 * n) % LANES, 1), quarter(found, n)
            )
            for n in range(4)
        ],
        axis=1,
    )


def gather_grid(arrivals, accs):
    names = ("xp", "xm", "yp", "ym", "zp", "zm")

    def body(*refs):
        kept = dict(zip(names, refs[:6]))
        own = refs[6 : 6 + len(accs)]
        velocity, faces, fluid_out, slots_out, rec = refs[6 + len(accs) :]
        for number, source in enumerate(consumed):
            rec[number * REC : (number + 1) * REC, :] = record(kept[source[0]], source[1])
            slots_out[number : number + 1, :] = slot_row(kept, source, None)
        rec[NBR_BINS * REC : 32 * REC, :] = jnp.zeros(((32 - NBR_BINS) * REC, LANES), jnp.float32)
        slots_out[NBR_BINS:32, :] = jnp.full((32 - NBR_BINS, LANES), -1.0, jnp.float32)
        hot = (
            slots_out[...] == lax.broadcasted_iota(jnp.int32, (32, LANES), 1).astype(jnp.float32)
        ).astype(jnp.float32)
        hot = jnp.transpose(hot)[:TPD, :].astype(jnp.bfloat16)
        received = jnp.concatenate([rec[pl.ds(r, 32, stride=REC), :] for r in range(REC)], axis=1)
        totals = pick(hot, received)
        for acc in own:
            totals = totals + jnp.concatenate(
                [acc[pl.ds(r, TPD, stride=REC), :] for r in range(REC)], axis=1
            )
        masses = totals[:, :CELLS]
        fluid = masses > 0.0
        safe = jnp.where(fluid, masses, 1.0)
        speeds = []
        for a in range(3):
            value = totals[:, (a + 1) * CELLS : (a + 2) * CELLS] / safe
            if a == 1:
                value = value - 0.5
            speeds.append(jnp.where(fluid, value, 0.0))
            velocity[:, a * CELLS : (a + 1) * CELLS] = speeds[a]
        faces[...] = pack_faces(speeds)
        fluid_out[...] = fluid.astype(jnp.float32)

    return call(
        body,
        "gather_grid",
        (*arrivals, *accs),
        (
            array(TPD, 3 * CELLS),
            array(TPD, FACES),
            array(TPD, CELLS),
            array(32, LANES),
        ),
        scratch_shapes=[pltpu.VMEM((32 * REC, LANES), jnp.float32)],
    )


def divergence(arrivals, code_row, code_column, velocity, faces, fluid, arrived):
    def body(*refs):
        payloads, code_row, code_column, fluid, velocity = refs[:6], *refs[6:10]
        fields = refs[10:17]
        hot_out, div_out, pressure = refs[17:]
        group = lax.broadcasted_iota(jnp.int32, (1, LANES), 1) // TPD
        codes = jnp.where(group == 0, code_row[0:1, :], -9999.0)
        for number, ref in enumerate(payloads):
            axis = number // 2
            which = (number + lax.axis_index(AXES[axis]) + 1) & 1
            slot = 1 + 3 * which + 2 - axis
            codes = jnp.where(group == slot, ref[META + GROUP : META + GROUP + 1, :], codes)
        hots = [
            (code_column[...] + float(step) == codes).astype(jnp.bfloat16) for step in face_codes
        ]
        hot = jnp.concatenate(hots, axis=0)
        hot_out[...] = hot
        total = None
        ghosts = [face_ghost(found, n) for n, found in enumerate(ghosts_of(hot, fields))]
        for a in range(3):
            own = velocity[:, a * CELLS : (a + 1) * CELLS]
            ahead, behind = ghosts[2 * a], ghosts[2 * a + 1]
            term = 0.5 * (beside(own, ahead, 2 * a) - beside(own, behind, 2 * a + 1))
            total = term if total is None else total + term
        div_out[...] = total
        pressure[...] = jnp.where(fluid[...] > 0.0, (0.0 - total) / 6.0, 0.0)

    field = array(TPD, CELLS)
    return call(
        body,
        "divergence",
        (*arrivals, code_row, code_column, fluid, velocity, faces, *arrived),
        (array(6 * TPD, LANES, dtype=jnp.bfloat16), field, field),
    )


def sweep(hot, div, fluid, pressure, arrived):
    def body(hot, div, fluid, *refs):
        fields, out = refs[:7], refs[7]
        values = fields[0][...]
        total = None
        for facing, ghost in enumerate(ghosts_of(hot[...], fields)):
            term = beside(values, ghost, facing)
            total = term if total is None else total + term
        out[...] = jnp.where(fluid[...] > 0.0, (total - div[...]) / 6.0, 0.0)

    return call(
        body,
        "sweep",
        (hot, div, fluid, pressure, *arrived),
        array(TPD, CELLS),
    )


def project(hot, fluid, velocity, slots, pressure, arrived):
    def body(hot, fluid, velocity, slots, *refs):
        fields = refs[:7]
        tiles, back_p, back_m, back_local, rec = refs[7:]
        values = fields[0][...]
        ghosts = ghosts_of(hot[...], fields)
        wet = fluid[...] > 0.0
        tiles[...] = jnp.zeros_like(tiles)
        rec[...] = jnp.zeros_like(rec)
        named = (
            slots[...] == lax.broadcasted_iota(jnp.int32, (32, LANES), 1).astype(jnp.float32)
        ).astype(jnp.bfloat16)[:, :TPD]
        for a in range(3):
            slope = 0.5 * (
                beside(values, ghosts[2 * a], 2 * a) - beside(values, ghosts[2 * a + 1], 2 * a + 1)
            )
            final = jnp.where(wet, velocity[:, a * CELLS : (a + 1) * CELLS] - slope, 0.0)
            copies = pick(named, final)
            for u in range(UPPER):
                row = a * UPPER + u
                tiles[pl.ds(row, TPD, stride=REC), :] = final[:, u * LANES : (u + 1) * LANES]
                rec[pl.ds(row, 32, stride=REC), :] = copies[:, u * LANES : (u + 1) * LANES]
        back_p[...] = rec[:META, :]
        back_m[...] = rec[META : 2 * META, :]
        back_local[...] = rec[2 * META : NBR_BINS * REC, :]

    block = array(META, LANES)
    return call(
        body,
        "project",
        (hot, fluid, velocity, slots, pressure, *arrived),
        (
            array(TPD * REC, LANES),
            block,
            block,
            array(8 * REC, LANES),
        ),
        scratch_shapes=[pltpu.VMEM((32 * REC, LANES), jnp.float32)],
    )


def results(tiles, pressure):
    def body(tiles, pressure, grid_out, pressure_out):
        for t in range(TPD):
            for u in range(UPPER):
                begin = t * CELLS + u * LANES
                grid_out[:, begin : begin + LANES] = tiles[pl.ds(t * REC + u, 3, stride=UPPER), :]
        for u in range(UPPER):
            pressure_out[pl.ds(u, TPD, stride=UPPER), :] = pressure[:, u * LANES : (u + 1) * LANES]

    return call(
        body,
        "results",
        (tiles, pressure),
        (array(3, TPD * CELLS), array(TPD * UPPER, LANES)),
    )


def sample_row(cell, tile, row, count):
    cells = cell[row : row + 1, :]
    upper = upper_index(cells, LANES, count)
    high = tile.astype(jnp.bfloat16)
    low = (tile - high.astype(jnp.float32)).astype(jnp.bfloat16)
    planes = lax.dot_general(
        jnp.concatenate([high, low], axis=0),
        one_hot(cells, LANES),
        (((1,), (0,)), ((), ())),
        preferred_element_type=jnp.float32,
    )
    planes = planes[:REC] + planes[REC:]
    wanted = (lax.broadcasted_iota(jnp.int32, (8, PPT), 0) & (UPPER - 1)) == upper
    sums = []
    for half in range(2):
        kept = jnp.where(wanted, planes[8 * half : 8 * half + 8], 0.0)
        kept = kept + pltpu.roll(kept, 7, 0)
        sums.append(kept + pltpu.roll(kept, 6, 0))
    return sums[0][0:1], sums[0][4:5], sums[1][0:1]


def store_row(out, row, values):
    for a in range(3):
        out[a, row : row + 1, :] = values[a]


particle_shape = jax.ShapeDtypeStruct((3, BINS, PPT), jnp.float32)


def sample_own(counts, slots, cell, tiles, sampled, start, blocks):
    def body(counts, slots, cell, tiles, *refs):
        out = refs[-1]
        base = (pl.program_id(0) + start) * 8
        for row in range(8):
            place = pl.multiple_of(slots[base + row] * REC, REC)
            tile = tiles[pl.ds(place, REC), :]
            store_row(out, row, sample_row(cell, tile, row, counts[base + row]))

    args = [counts, slots, cell, near(tiles)]
    specs = [
        scalars(),
        scalars(),
        pl.BlockSpec((8, PPT), lambda i: (i + start, 0)),
        held(),
    ]
    alias = {}
    if sampled is not None:
        args.append(sampled)
        specs.append(pl.BlockSpec(memory_space=pl.ANY))
        alias = {4: 0}
    return call(
        body,
        "sample_own",
        tuple(args),
        particle_shape,
        flops=blocks * 8 * 2_000_000,
        grid=(blocks,),
        in_specs=specs,
        out_specs=pl.BlockSpec((3, 8, PPT), lambda i: (0, i + start, 0)),
        input_output_aliases=alias,
    )


def sample_middle(counts, cell, buffers):
    names = ("yp", "ym", "zp", "zm")

    def body(counts, cell, *refs):
        held_by = dict(zip(names, refs))
        out = refs[len(names)]
        for block, rows in middle_rows.items():
            for row in rows:
                number = block * 8 + row
                name, index = final_sources[number]
                tile = record(held_by[name], index)
                values = sample_row(cell, tile, number, counts[OWN_BINS + number])
                store_row(out, number - GROUP, values)

    return call(
        body,
        "sample_middle",
        (counts, near(cell), *[near(buffer) for buffer in buffers]),
        array(3, 8, PPT),
        flops=8 * 2_000_000,
        in_specs=[scalars()] + [held()] * (1 + len(names)),
        out_specs=held(),
    )


def sample_sides(counts, cell, buffers, middle, sampled):
    def body(counts, cell, xp, xm, middle, sampled, out, buffer, sent):
        held_by = {"xp": xp, "xm": xm}
        copies = []
        for block in (0, 2, 1, 3):
            for row in side_rows[block]:
                number = block * 8 + row
                name, index = final_sources[number]
                tile = record(held_by[name], index)
                store_row(
                    buffer, number, sample_row(cell, tile, number, counts[OWN_BINS + number])
                )
            for row in middle_rows.get(block, ()):
                number = block * 8 + row
                index = number - GROUP
                store_row(buffer, number, [middle[a, index : index + 1, :] for a in range(3)])
            copy = pltpu.make_async_copy(
                buffer.at[:, pl.ds(8 * block, block_rows[block])],
                out.at[:, pl.ds(OWN_BINS + 8 * block, block_rows[block])],
                sent.at[block],
            )
            copy.start()
            copies.append(copy)
        for copy in copies:
            copy.wait()

    return call(
        body,
        "sample_sides",
        (counts, *[near(value) for value in (cell, *buffers, middle)], sampled),
        particle_shape,
        flops=18 * 2_000_000,
        in_specs=[scalars()] + [held()] * 4 + [pl.BlockSpec(memory_space=pl.ANY)],
        out_specs=pl.BlockSpec(memory_space=pl.ANY),
        input_output_aliases={5: 0},
        scratch_shapes=[pltpu.VMEM((3, 32, PPT), jnp.float32), pltpu.SemaphoreType.DMA((4,))],
    )


def exchange(values):
    return [swap(values, axis, which) for which in (0, 1) for axis in reversed(AXES)]


def together(*values):
    return lax.optimization_barrier(values)


def with_kept(sources):
    return [("kept", n - 18) if name == "rec" else (name, n) for name, n in sources]


def local(tile_coords, owner_map, bin_tile, counts, cell, offset, velocity, affine, mass):
    parts = (
        cell,
        jnp.transpose(offset, (1, 0, 2)),
        jnp.transpose(velocity, (1, 0, 2)),
        jnp.transpose(affine, (1, 0, 2)),
        mass,
    )
    slots, code_row, code_column, slot_rows, below, above = splat_sides(
        tile_coords, owner_map, bin_tile, counts, parts
    )
    xp, xm = ring(above, "gx", 1), ring(below, "gx", -1)
    middle = splat_middle(counts, slots, parts)
    up, down = forward(
        ("mid", "xp", "xm"),
        (middle, xp, xm),
        slot_rows,
        code_row,
        (y_sources(1), y_sources(-1)),
        "forward_y",
    )
    slots, up, down = together(slots, up, down)
    yp, ym = ring(up, "gy", 1), ring(down, "gy", -1)
    acc_y = splat_own(counts, slots, parts, 0, 2)
    yp, ym, acc_y = together(yp, ym, acc_y)
    up, down = forward(
        ("mid", "xp", "xm", "yp", "ym"),
        (middle, xp, xm, yp, ym),
        slot_rows,
        code_row,
        (z_sources(1), z_sources(-1)),
        "forward_z",
    )
    slots, up, down = together(slots, up, down)
    zp, zm = ring(up, "gz", 1), ring(down, "gz", -1)
    acc_z = splat_own(counts, slots, parts, 2, 2)
    arrivals = (xp, xm, yp, ym, zp, zm)
    grid_u, faces, fluid, nbr_slots = gather_grid(arrivals, (acc_y, acc_z))
    hot, div, pressure = divergence(
        arrivals, code_row, code_column, grid_u, faces, fluid, exchange(faces)
    )
    for _ in range(SWEEPS - 1):
        pressure = sweep(hot, div, fluid, pressure, exchange(pressure))
    leaving = lax.slice_in_dim(together(cell, div)[0], OWN_BINS, BINS, axis=0)
    tiles, back_p, back_m, kept = project(
        hot, fluid, grid_u, nbr_slots, pressure, exchange(pressure)
    )
    rzp, rzm = ring(back_p, "gz", -1), ring(back_m, "gz", 1)
    sampled = sample_own(counts, slots, cell, tiles, None, 0, 2)
    rzp, rzm, sampled = together(rzp, rzm, sampled)
    up, down = reply(
        ("kept", "zp", "zm"),
        (kept, rzp, rzm),
        (with_kept(y_reply_sources(1)), with_kept(y_reply_sources(-1))),
        "reply_y",
    )
    slots, up, down = together(slots, up, down)
    ryp, rym = ring(up, "gy", -1), ring(down, "gy", 1)
    sampled = sample_own(counts, slots, cell, tiles, sampled, 2, 2)
    ryp, rym, sampled = together(ryp, rym, sampled)
    up, down = reply(
        ("kept", "zp", "zm", "yp", "ym"),
        (kept, rzp, rzm, ryp, rym),
        (with_kept(x_reply_sources(1)), with_kept(x_reply_sources(-1))),
        "reply_x",
    )
    slots, up, down = together(slots, up, down)
    rxp, rxm = ring(up, "gx", -1), ring(down, "gx", 1)
    middle = sample_middle(counts, leaving, (ryp, rym, rzp, rzm))
    grid_v, final_pressure = results(tiles, pressure)
    sampled = sample_sides(counts, leaving, (rxp, rxm), middle, sampled)
    return grid_v, final_pressure.reshape(-1), jnp.transpose(sampled, (1, 0, 2))


def solution(mesh):
    split = P(AXES)
    particles = P(AXES, None, None)
    return jax.shard_map(
        local,
        mesh=mesh,
        in_specs=(
            P(None, AXES),
            P(),
            split,
            split,
            P(AXES, None),
            particles,
            particles,
            particles,
            P(AXES, None),
        ),
        out_specs=(P(None, AXES), split, particles),
        check_vma=False,
    )
```
